32 devices in a mesh: depth: 8 (over z, core), tile: 4 (over y, x).
Axes of the slice: x: 2, y: 2, z: 4, core: 2. Of those that a mesh axis runs over, the one named last changes fastest.
Arguments:
- potential: float32 [8, 1024, 384], P('depth', 'tile'), may hold values from 0 to 3
- probe: bfloat16 [2, 256, 256], replicated, may hold values from -6 to 6
- positions: int32 [4, 19, 2], P('tile'), may hold values from 0 to 128
- intensity: bfloat16 [4, 4, 256, 256], P('tile'), may hold values from 0.099609375 to 3
- fwd_wave: float32 [8, 4, 2, 256, 256], P('depth', 'tile'), may hold values from -6 to 6
- adj_wave: bfloat16 [8, 4, 2, 256, 256], P('depth', 'tile'), may hold values from -6 to 6
- saved_wave: bfloat16 [8, 4, 4, 2, 256, 256], P('depth', 'tile'), may hold values from -6 to 6
Outputs:
- fwd_next: float32 [8, 4, 2, 256, 256], P('depth', 'tile')
- adj_next: bfloat16 [8, 4, 2, 256, 256], P('depth', 'tile')
- gradient: float32 [8, 1024, 384], P('depth', 'tile')
The draws below stay inside these ranges and needn't reach their ends.
Inputs may be any that keep to these rules, and one draw needn't show every extreme that they name: `positions`: window corners keep the whole window inside the tile's extent.
All inputs are finite; a program needn't handle non-finite values.
Results may differ from the reference program's by a relative error of at most 0.04.
Values may be sent and summed in bfloat16 or wider, within the bound.
A program may use at most 64 MiB of HBM per device.

```python
import math
import jax
import jax.numpy as jnp
from jax import lax

WAVE = 256
CORE = 256
MARGIN = 64
TICKS = 4
TILE = 384
SLICES = 8
WIDTH = 1024
MICRO = 19
N_DEPTH = 8
N_TILE = 4


def with_ends(drawn, own_key, low, high):
    spot = [jax.random.randint(jax.random.fold_in(own_key, axis), (), 0, length) for axis, length in enumerate(drawn.shape)]
    main_axis = drawn.shape.index(max(drawn.shape))
    next_to = spot[:main_axis] + [(spot[main_axis] + 1) % drawn.shape[main_axis]] + spot[main_axis + 1:]
    return drawn.at[tuple(spot)].set(low).at[tuple(next_to)].set(high)


def level_of(key, dims, shards, low, top_value):
    loudness = 1.0
    for dim, blocks in shards:
        draws = jax.random.uniform(jax.random.fold_in(jax.random.fold_in(key, 6), dim), (blocks,), jnp.float32, low / len(shards), top_value / len(shards))
        loudness = loudness * jnp.repeat(jnp.exp(draws), dims[dim] // blocks).reshape((-1,) + (1,) * (len(dims) - 1 - dim))
    return loudness


def noise(key, shape, scale, bound, cuts=(), kind=jnp.bfloat16):
    factor_of = level_of(key, shape, cuts, -0.22, 0.18) if cuts else 1.0
    entries = jax.random.normal(key, shape, jnp.float32) * scale * factor_of
    return jnp.minimum(jnp.maximum(entries, -bound), bound).astype(kind)


def setup_inputs(seed: int = 0) -> dict:
    key_of = jax.random.split(jax.random.key(seed), 8)
    return {
        "potential": jnp.clip(3.0 * jax.random.uniform(key_of[0], (SLICES, WIDTH, TILE), jnp.float32) ** level_of(key_of[0], (SLICES, WIDTH, TILE), ((0, 8), (1, 4)), -0.2, 0.2), 0.0, 3.0),
        "probe": noise(key_of[1], (2, WAVE, WAVE), 1.0, 6.0),
        "positions": with_ends(jax.random.randint(key_of[2], (N_TILE, MICRO, 2), 0, TILE - WAVE + 1), jax.random.fold_in(key_of[2], 1), 0, TILE - WAVE).astype(jnp.int32),
        "intensity": jnp.clip(jnp.exp(math.log(3.0) - 3.4051113 * jax.random.uniform(key_of[3], (N_TILE, TICKS, WAVE, WAVE), jnp.float32) ** level_of(key_of[3], (N_TILE, TICKS, WAVE, WAVE), ((0, 4),), -0.2, 0.2)), 0.099609375, 3.0).astype(jnp.bfloat16),
        "fwd_wave": noise(key_of[4], (SLICES, N_TILE, 2, WAVE, WAVE), 1.0, 6.0, ((0, 8), (1, 4)), jnp.float32),
        "adj_wave": noise(key_of[5], (SLICES, N_TILE, 2, WAVE, WAVE), 1.0, 6.0, ((0, 8), (1, 4))),
        "saved_wave": noise(key_of[6], (SLICES, N_TILE, TICKS, 2, WAVE, WAVE), 1.0, 6.0, ((0, 8), (1, 4))),
    }


SIGMA = 0.8
DEFOCUS = 6.0

def tables(n):
    idx = jnp.arange(n, dtype=jnp.int32)
    prod = idx[:, None] * idx[None, :] % n
    angle = prod.astype(jnp.float32) * (2.0 * math.pi / n)
    scale = 1.0 / math.sqrt(n)
    return ((jnp.cos(angle) * scale).astype(jnp.bfloat16), (jnp.sin(angle) * scale).astype(jnp.bfloat16))

def propagator(n):
    idx = jnp.arange(n, dtype=jnp.int32)
    freq = jnp.where(idx < n // 2, idx, idx - n).astype(jnp.float32)
    square = freq[:, None] * freq[:, None] + freq[None, :] * freq[None, :]
    phase = -math.pi * DEFOCUS * square / (n * n)
    return (jnp.cos(phase), jnp.sin(phase))

def to_half(value):
    return lax.optimization_barrier(value.astype(jnp.bfloat16)).astype(jnp.float32)

def product(left, right):
    return jnp.dot(left, right, precision=lax.Precision.HIGHEST)

def transform(real, imag, cos_t, sin_t, sign):
    xr = to_half(real)
    xi = to_half(imag)
    ar = product(cos_t, xr) + sign * product(sin_t, xi)
    ai = product(cos_t, xi) - sign * product(sin_t, xr)
    ar = to_half(ar)
    ai = to_half(ai)
    br = product(ar, cos_t) + sign * product(ai, sin_t)
    bi = product(ai, cos_t) - sign * product(ar, sin_t)
    return (br, bi)

def forward_section(wave, window, intens, is_last, cos_t, sin_t, prop_r, prop_i):
    trans_r = jnp.cos(SIGMA * window)
    trans_i = jnp.sin(SIGMA * window)
    ur = trans_r * wave[0] - trans_i * wave[1]
    ui = trans_r * wave[1] + trans_i * wave[0]
    big_r, big_i = transform(ur, ui, cos_t, sin_t, 1.0)
    far_r = big_r * prop_r - big_i * prop_i
    far_i = big_r * prop_i + big_i * prop_r
    excess = far_r * far_r + far_i * far_i - intens.astype(jnp.float32)
    src_r = jnp.where(is_last, excess * far_r, far_r)
    src_i = jnp.where(is_last, excess * far_i, far_i)
    out_r, out_i = transform(src_r, src_i, cos_t, sin_t, -1.0)
    return jnp.stack([out_r, out_i])

def backward_section(adjoint, saved, window, cos_t, sin_t, prop_r, prop_i):
    lr, li = transform(adjoint[0].astype(jnp.float32), adjoint[1].astype(jnp.float32), cos_t, sin_t, 1.0)
    mr = lr * prop_r + li * prop_i
    mi = li * prop_r - lr * prop_i
    lur, lui = transform(mr, mi, cos_t, sin_t, -1.0)
    trans_r = jnp.cos(SIGMA * window)
    trans_i = jnp.sin(SIGMA * window)
    saved_r = saved[0].astype(jnp.float32)
    saved_i = saved[1].astype(jnp.float32)
    uar = trans_r * saved_r - trans_i * saved_i
    uai = trans_r * saved_i + trans_i * saved_r
    delta = SIGMA * (lui * uar - lur * uai)
    back = jnp.stack([trans_r * lur + trans_i * lui, trans_r * lui - trans_i * lur])
    return (back, delta)

def reference(potential, probe, positions, intensity, fwd_wave, adj_wave, saved_wave):
    n = WAVE
    sections = N_DEPTH
    tiles = N_TILE
    core = CORE
    margin = MARGIN
    cos_h, sin_h = tables(n)
    cos_t = cos_h.astype(jnp.float32)
    sin_t = sin_h.astype(jnp.float32)
    prop_r, prop_i = propagator(n)
    padded = jnp.pad(potential, ((0, 0), (margin, margin), (0, 0)))
    section_ids = jnp.arange(sections, dtype=jnp.int32)
    last_mask = section_ids == sections - 1
    probe_wave = probe.astype(jnp.float32)

    def cut(extent, corner):
        return lax.dynamic_slice(extent, (corner[0], corner[1]), (n, n))

    def place(grad, delta, corner):
        old = lax.dynamic_slice(grad, (corner[0], corner[1]), (n, n))
        return lax.dynamic_update_slice(grad, old + delta, (corner[0], corner[1]))

    def one_tile(inputs):
        tile_index, spots, intens, wave, adjoint, saved = inputs
        start = (tile_index * core).astype(jnp.int32)
        extent = lax.dynamic_slice(padded, (jnp.int32(0), start, jnp.int32(0)), (sections, core + 2 * margin, TILE))
        grad = jnp.zeros((sections, core + 2 * margin, TILE), jnp.float32)
        for tick in range(TICKS):
            f_pos = spots[tick - section_ids + 2 * sections - 1]
            a_pos = spots[tick + section_ids]
            f_win = jax.vmap(cut)(extent, f_pos)
            a_win = jax.vmap(cut)(extent, a_pos)
            sent = jax.vmap(lambda w, v, last: forward_section(w, v, intens[tick], last, cos_t, sin_t, prop_r, prop_i))(wave, f_win, last_mask)
            back, delta = jax.vmap(lambda a, s, v: backward_section(a, s, v, cos_t, sin_t, prop_r, prop_i))(adjoint, saved[:, tick], a_win)
            grad = jax.vmap(place)(grad, delta, a_pos)
            wave = jnp.concatenate([probe_wave[None], sent[:-1]], 0)
            adjoint = jnp.concatenate([back[1:], sent[-1:]], 0).astype(jnp.bfloat16)
        return (wave, adjoint, grad)
    tile_ids = jnp.arange(tiles, dtype=jnp.int32)
    waves, adjoints, grads = lax.map(one_tile, (tile_ids, positions, intensity, jnp.swapaxes(fwd_wave, 0, 1), jnp.swapaxes(adj_wave, 0, 1), jnp.swapaxes(saved_wave, 0, 1)))
    inner = grads[:, :, margin:margin + core]
    zeros = jnp.zeros((1, sections, margin, TILE), jnp.float32)
    from_left = jnp.concatenate([zeros, grads[:-1, :, margin + core:]], 0)
    from_right = jnp.concatenate([grads[1:, :, :margin], zeros], 0)
    inner = inner + jnp.pad(from_left, ((0, 0), (0, 0), (0, core - margin), (0, 0)))
    inner = inner + jnp.pad(from_right, ((0, 0), (0, 0), (core - margin, 0), (0, 0)))
    gradient = jnp.swapaxes(inner, 0, 1).reshape(sections, tiles * core, TILE)
    return (jnp.swapaxes(waves, 0, 1), jnp.swapaxes(adjoints, 0, 1), gradient)
```

```python
import functools
import math

import jax
import jax.numpy as jnp
import numpy as np
from jax import lax
from jax.experimental import pallas as pl
from jax.experimental.pallas import tpu as pltpu
from jax.sharding import PartitionSpec as P

SIGMA = 0.8
DEFOCUS = 6.0
VTOP = 3.0
ROWS = 128
LANES = 128
STEP = 32
VLIM = 40
MESH = pl.DeviceIdType.MESH
F32 = jnp.float32
BF16 = jnp.bfloat16


def rounded(x):
    return x.real.astype(BF16).astype(np.float64) + 1j * x.imag.astype(BF16).astype(np.float64)


def left_blocks(x):
    n = x.shape[0]
    nc = n // ROWS
    out = np.zeros((nc, nc, 2 * ROWS, 2 * ROWS))
    for o in range(nc):
        for c in range(nc):
            b = x[o * ROWS : (o + 1) * ROWS, c * ROWS : (c + 1) * ROWS]
            out[o, c] = np.block([[b.real, -b.imag], [b.imag, b.real]])
    return out.transpose(0, 2, 1, 3).reshape(2 * n, 2 * n)


def right_block(x):
    return np.block([[x.real, x.imag], [-x.imag, x.real]])


def tables(n):
    idx = np.arange(n)
    angle = (idx[:, None] * idx[None, :] % n) * (2.0 * math.pi / n)
    scale = 1.0 / math.sqrt(n)
    cos_t = np.asarray((np.cos(angle) * scale).astype(BF16)).astype(np.float64)
    sin_t = np.asarray((np.sin(angle) * scale).astype(BF16)).astype(np.float64)
    freq = np.where(idx < n // 2, idx, idx - n).astype(np.float64)
    q = np.exp(-1j * math.pi * DEFOCUS * freq * freq / (n * n))
    f = cos_t - 1j * sin_t
    m = (np.conj(f) * q[None, :]) @ f
    m = (m + m.T) / 2
    best = (np.inf, 1.0)
    for size in np.linspace(0.7, 1.4, 64):
        z = (size * np.exp(1j * np.linspace(0.0, math.pi / 2, 128, endpoint=False)))[:, None]
        row = m[0][None, :]
        miss = np.sum(np.abs(rounded(row * z) - row * z) ** 2, axis=1) / size**2
        miss += np.sum(np.abs(rounded(row / z) - row / z) ** 2, axis=1) * size**2
        at = int(np.argmin(miss))
        if miss[at] < best[0]:
            best = (miss[at], z[at, 0])
    z = best[1]
    g = np.conj(f) * q[None, :]
    main = np.stack([left_blocks(z * m), right_block(m / z)]).astype(BF16)
    ends = [p for v in (f, g, g.T) for p in (v.real, v.imag)]
    return main, np.stack(ends).astype(BF16)


def sin_cos(v):
    mid = 0.5 * VTOP * SIGMA
    y = v * SIGMA - mid
    z = y * y
    s = y * (1.0 + z * (-1.0 / 6 + z * (1.0 / 120 + z * (-1.0 / 5040 + z * (1.0 / 362880)))))
    c = 1.0 + z * (-0.5 + z * (1.0 / 24 + z * (-1.0 / 720 + z * (1.0 / 40320))))
    sm, cm = math.sin(mid), math.cos(mid)
    return s * cm + c * sm, c * cm - s * sm


def dot(a, b):
    return jnp.dot(a, b, preferred_element_type=F32)


def kernel(
    sections, tiles,
    pos, pot_h, probe_h, inten_h, fwd_h, adj_h, saved_h, main_h, ends_h,
    o_fwd, o_adj, o_grad,
    in_f, in_b, out_f, out_b, main, l_f, r_f, l_g, r_g,
    cs, tf, ta, bk, total, pad, y_buf,
    halo_out, halo_in, edge_out, edge_in,
    pot, probe, inten, fwd, adj, saved, ends, load_sem,
    send_f, recv_f, send_b, recv_b, send_h, recv_h, send_e, recv_e,
):
    n = probe.shape[1]
    nc = n // ROWS
    cols = n // LANES
    core, width = pot.shape[1], pot.shape[2]
    margin = (width - core) // 2
    ticks = inten.shape[1]
    s = lax.axis_index("depth")
    t = lax.axis_index("tile")
    first, last = s == 0, s == sections - 1
    low, high = t == 0, t == tiles - 1

    loads = {}

    def load(name, src, dst):
        loads[name] = pltpu.make_async_copy(src, dst, load_sem.at[len(loads)])
        return loads[name]

    load("pot", pot_h, pot).start()
    barrier = pltpu.get_barrier_semaphore()
    one = lambda c: jnp.where(c, 1, 0).astype(jnp.int32)

    def greet(cond, axis, to):
        @pl.when(cond)
        def _():
            pl.semaphore_signal(barrier, inc=1, device_id={axis: to}, device_id_type=MESH)

    greet(t > 0, "tile", t - 1)
    greet(t < tiles - 1, "tile", t + 1)
    greet(s > 0, "depth", s - 1)
    greet(s < sections - 1, "depth", s + 1)
    load("main", main_h, main).start()
    load("adj", adj_h, adj).start()
    load("fwd", fwd_h, fwd).start()
    load("probe", probe_h, probe)
    load("ends", ends_h, ends)
    load("inten", inten_h, inten)

    @pl.when(first)
    def _():
        loads["probe"].start()

    @pl.when(last)
    def _():
        loads["ends"].start()
        loads["inten"].start()

    load("saved", saved_h, saved).start()
    loads["pot"].wait()
    halo_out[0] = pot[0, 0:margin, :].astype(BF16)
    halo_out[1] = pot[0, core - margin : core, :].astype(BF16)
    pl.semaphore_wait(barrier, one(s > 0) + one(s < sections - 1) + one(t > 0) + one(t < tiles - 1))

    def hop(src, dst, ssem, rsem, axis, to):
        return pltpu.make_async_remote_copy(
            src_ref=src, dst_ref=dst, send_sem=ssem, recv_sem=rsem,
            device_id={axis: to}, device_id_type=MESH,
        )

    def tile_pair(src, dst, ssem, rsem):
        down = hop(src.at[0], dst.at[1], ssem.at[0], rsem.at[1], "tile", t - 1)
        up = hop(src.at[1], dst.at[0], ssem.at[1], rsem.at[0], "tile", t + 1)
        return down, up

    def tile_start(src, dst, ssem, rsem):
        down, up = tile_pair(src, dst, ssem, rsem)
        pl.when(t > 0)(down.start)
        pl.when(t < tiles - 1)(up.start)

    def tile_wait(src, dst, ssem, rsem):
        down, up = tile_pair(src, dst, ssem, rsem)

        @pl.when(t > 0)
        def _():
            down.wait_send()
            up.wait_recv()

        @pl.when(t < tiles - 1)
        def _():
            up.wait_send()
            down.wait_recv()

    tile_start(halo_out, halo_in, send_h, recv_h)

    def stacked(x):
        return x.reshape(2 * ROWS, n)

    def m_left(o, c):
        return main[0, o * 2 * ROWS : (o + 1) * 2 * ROWS, c * 2 * ROWS : (c + 1) * 2 * ROWS]

    def product(get_left, get_x, r_ref, sink):
        acc = [None] * nc
        for c in range(nc):
            x = get_x(c)
            for o in range(nc):
                term = dot(get_left(o, c), x)
                acc[o] = term if acc[o] is None else acc[o] + term
        for o in range(nc):
            a = acc[o].astype(BF16)
            out = dot(jnp.concatenate([a[0:ROWS, :], a[ROWS : 2 * ROWS, :]], axis=1), r_ref[...])
            sink(o, out[:, 0:n], out[:, n : 2 * n])

    loads["adj"].wait()
    for c in range(nc):
        rows = slice(c * ROWS, (c + 1) * ROWS)
        in_b[0, c, 0] = adj[0, 0, 0, rows, :]
        in_b[0, c, 1] = -adj[0, 0, 1, rows, :]
    loads["main"].wait()

    def keep(o, lur, lui):
        rows = slice(o * ROWS, (o + 1) * ROWS)
        bk[0, rows, :] = lur
        bk[1, rows, :] = lui

    product(m_left, lambda c: stacked(in_b[0, c]), main.at[1], keep)

    def table(src, dst, count):
        for at in range(0, count, STEP):
            sv, cv = sin_cos(src(at))
            for i in range(cols + 1):
                one_tile = slice(i * LANES, (i + 1) * LANES)
                cs[i, pl.ds(2 * (dst + at), STEP, stride=2), :] = cv[:, one_tile]
                cs[i, pl.ds(2 * (dst + at) + 1, STEP, stride=2), :] = sv[:, one_tile]

    table(lambda at: pot[0, at : at + STEP, :], margin, core)
    total[...] = jnp.zeros_like(total)
    spare = width - n
    for i in range(cols + 1):
        pad[i, 0 : 2 * spare, :] = jnp.zeros((2 * spare, LANES), F32)
        pad[i, 2 * (spare + n) :, :] = jnp.zeros((2 * spare, LANES), F32)
    loads["fwd"].wait()
    for c in range(nc):
        rows = slice(c * ROWS, (c + 1) * ROWS)
        for part in range(2):
            in_f[0, c, part] = fwd[0, 0, part, rows, :].astype(BF16)

    @pl.when(first)
    def _():
        loads["probe"].wait()
        for k in range(ticks - 1):
            for c in range(nc):
                for part in range(2):
                    in_f[k + 1, c, part] = probe[part, c * ROWS : (c + 1) * ROWS, :]
        for part in range(2):
            o_fwd[0, 0, part] = probe[part]

    @pl.when(last)
    def _():
        loads["ends"].wait()
        loads["inten"].wait()

        def fill_left(ref, xr, xi):
            for o in range(nc):
                for c in range(nc):
                    br = xr[o * ROWS : (o + 1) * ROWS, c * ROWS : (c + 1) * ROWS]
                    bi = xi[o * ROWS : (o + 1) * ROWS, c * ROWS : (c + 1) * ROWS]
                    ref[o, c, 0:ROWS, 0:ROWS] = br
                    ref[o, c, 0:ROWS, ROWS : 2 * ROWS] = -bi
                    ref[o, c, ROWS : 2 * ROWS, 0:ROWS] = bi
                    ref[o, c, ROWS : 2 * ROWS, ROWS : 2 * ROWS] = br

        def fill_right(ref, xr, xi):
            ref[0:n, 0:n] = xr
            ref[0:n, n : 2 * n] = xi
            ref[n : 2 * n, 0:n] = -xi
            ref[n : 2 * n, n : 2 * n] = xr

        fill_left(l_f, ends[0], ends[1])
        fill_right(r_f, ends[0], ends[1])
        fill_left(l_g, ends[2], ends[3])
        fill_right(r_g, ends[4], ends[5])

    @pl.when(low)
    def _():
        halo_in[0] = jnp.zeros((margin, width), BF16)
        edge_in[0] = jnp.zeros((margin, width), BF16)

    @pl.when(high)
    def _():
        halo_in[1] = jnp.zeros((margin, width), BF16)
        edge_in[1] = jnp.zeros((margin, width), BF16)

    tile_wait(halo_out, halo_in, send_h, recv_h)
    table(lambda at: halo_in[0, at : at + STEP, :].astype(F32), 0, margin)
    table(lambda at: halo_in[1, at : at + STEP, :].astype(F32), margin + core, margin)

    lane = lax.broadcasted_iota(jnp.int32, (STEP, LANES), 1)

    def window(index, out, slot):
        r, c = pos[0, 0, index], pos[0, 1, index]
        turn = lax.rem(LANES - c, LANES)
        own = lane < LANES - c
        for part in range(2):
            for at in range(0, n, STEP):
                rows = pl.ds(2 * (r + at) + part, STEP, stride=2)
                x = [pltpu.roll(cs[i, rows, :], turn, 1) for i in range(cols + 1)]
                for i in range(cols):
                    out[slot, part, at : at + STEP, i * LANES : (i + 1) * LANES] = jnp.where(own, x[i], x[i + 1])

    def windows(k):
        window(k + s, ta, lax.rem(k, 2))
        window(k - s + 2 * sections - 1, tf, lax.rem(k, 2))

    def scatter(k):
        r, c = pos[0, 0, k + s], pos[0, 1, k + s]
        own = lane >= c
        turn = lax.rem(c, LANES)
        for at in range(0, n, STEP):
            rows = slice(at, at + STEP)
            sr = saved[0, 0, k, 0, rows, :].astype(F32)
            si = saved[0, 0, k, 1, rows, :].astype(F32)
            d = (bk[1, rows, :] * sr + bk[0, rows, :] * si) * -SIGMA
            d = [pltpu.roll(d[:, i * LANES : (i + 1) * LANES], turn, 1) for i in range(cols)]
            zero = jnp.zeros((STEP, LANES), F32)
            d = [zero] + d + [zero]
            for i in range(cols + 1):
                pad[i, pl.ds(2 * (spare + at), STEP, stride=2), :] = jnp.where(own, d[i + 1], d[i])
        for at in range(0, width, STEP):
            for i in range(cols + 1):
                total[at : at + STEP, i * LANES : (i + 1) * LANES] += pad[i, pl.ds(2 * (spare - r + at), STEP, stride=2), :]

    def copy_f(k, c):
        return hop(out_f.at[k, c], in_f.at[k + 1, c], send_f.at[k, c], recv_f.at[k, c], "depth", s + 1)

    def copy_b(k, c):
        return hop(out_b.at[k, c], in_b.at[k + 1, c], send_b.at[k, c], recv_b.at[k, c], "depth", s - 1)

    def send_back(k, c, lur, lui):
        rows = slice(c * ROWS, (c + 1) * ROWS)
        slot = lax.rem(k, 2)
        tr, ti = ta[slot, 0, rows, :], ta[slot, 1, rows, :]
        br = tr * lur - ti * lui
        bi = tr * lui + ti * lur
        bk[0, rows, :] = br
        bk[1, rows, :] = bi
        out_b[k, c, 0] = br.astype(BF16)
        out_b[k, c, 1] = bi.astype(BF16)

        @pl.when(jnp.logical_not(first))
        def _():
            copy_b(k, c).start()

    def backward(k):
        def arrived(c):
            @pl.when(jnp.logical_not(last))
            def _():
                copy_b(k - 1, c).wait_recv()
            return stacked(in_b[k, c])

        product(m_left, arrived, main.at[1], functools.partial(send_back, k))

    def entering(k, c, waits):
        if waits:
            @pl.when(jnp.logical_not(first))
            def _():
                copy_f(k - 1, c).wait_recv()
        rows = slice(c * ROWS, (c + 1) * ROWS)
        slot = lax.rem(k, 2)
        wr, wi = in_f[k, c, 0].astype(F32), in_f[k, c, 1].astype(F32)
        tr, ti = tf[slot, 0, rows, :], tf[slot, 1, rows, :]
        return jnp.concatenate([tr * wr - ti * wi, tr * wi + ti * wr], axis=0).astype(BF16)

    def forward(k, waits=True):
        def sink(c, outr, outi):
            out_f[k, c, 0] = outr.astype(BF16)
            out_f[k, c, 1] = outi.astype(BF16)
            copy_f(k, c).start()

        product(m_left, lambda c: entering(k, c, waits), main.at[1], sink)

    def forward_last(k, waits=True):
        def detect(c, vr, vi):
            rows = slice(c * ROWS, (c + 1) * ROWS)
            excess = vr * vr + vi * vi - inten[0, k, rows, :].astype(F32)
            y_buf[c, 0:ROWS, :] = (excess * vr).astype(BF16)
            y_buf[c, ROWS : 2 * ROWS, :] = (excess * vi).astype(BF16)

        def seed(c, outr, outi):
            in_b[k + 1, c, 0] = outr.astype(BF16)
            in_b[k + 1, c, 1] = -outi.astype(BF16)

        product(lambda o, c: l_f[o, c], lambda c: entering(k, c, waits), r_f, detect)
        product(lambda o, c: l_g[o, c], lambda c: y_buf[c], r_g, seed)

    windows(0)
    for c in range(nc):
        rows = slice(c * ROWS, (c + 1) * ROWS)
        send_back(0, c, bk[0, rows, :], bk[1, rows, :])

    @pl.when(jnp.logical_not(last))
    def _():
        forward(0, False)

    @pl.when(last)
    def _():
        forward_last(0, False)

    windows(1)
    loads["saved"].wait()
    scatter(0)

    early = jnp.logical_or(first, jnp.logical_and(lax.rem(s, 2) == 1, jnp.logical_not(last)))

    @pl.when(early)
    def _():
        def tick(k, carry):
            forward(k)

            @pl.when(k < ticks - 1)
            def _():
                windows(k + 1)
            backward(k)
            scatter(k)
            return carry
        lax.fori_loop(1, ticks, tick, 0)

    @pl.when(jnp.logical_not(early))
    def _():
        def tick(k, carry):
            backward(k)
            scatter(k)

            @pl.when(k < ticks - 1)
            def _():
                windows(k + 1)

            @pl.when(jnp.logical_not(last))
            def _():
                forward(k)

            @pl.when(last)
            def _():
                forward_last(k)
            return carry
        lax.fori_loop(1, ticks, tick, 0)

    edge_out[0] = total[0:margin, :].astype(BF16)
    edge_out[1] = total[margin + core :, :].astype(BF16)
    tile_start(edge_out, edge_in, send_e, recv_e)
    o_grad[0, margin : core - margin, :] = total[2 * margin : core, :]
    tile_wait(edge_out, edge_in, send_e, recv_e)
    o_grad[0, 0:margin, :] = total[margin : 2 * margin, :] + edge_in[0].astype(F32)
    o_grad[0, core - margin : core, :] = total[core : core + margin, :] + edge_in[1].astype(F32)
    for c in range(nc):
        rows = slice(c * ROWS, (c + 1) * ROWS)

        @pl.when(jnp.logical_not(last))
        def _():
            copy_b(ticks - 1, c).wait_recv()
        o_adj[0, 0, :, rows, :] = in_b[ticks, c]

        @pl.when(jnp.logical_not(first))
        def _():
            copy_f(ticks - 1, c).wait_recv()
            o_fwd[0, 0, :, rows, :] = in_f[ticks, c]
    for k in range(ticks):
        for c in range(nc):
            @pl.when(jnp.logical_not(last))
            def _():
                copy_f(k, c).wait_send()

            @pl.when(jnp.logical_not(first))
            def _():
                copy_b(k, c).wait_send()


def finish(wave, adj, grad, o_wave, o_adj, o_grad, wave_buf, adj_buf, sem):
    moves = [pltpu.make_async_copy(grad, o_grad, sem.at[0])]
    moves[0].start()
    for part in range(2):
        wave_buf[0, 0, part] = wave[0, 0, part].astype(F32)
        move = pltpu.make_async_copy(wave_buf.at[0, 0, part], o_wave.at[0, 0, part], sem.at[1 + part])
        move.start()
        moves.append(move)
    adj_buf[0, 0, 0] = adj[0, 0, 0]
    adj_buf[0, 0, 1] = -adj[0, 0, 1]
    moves.append(pltpu.make_async_copy(adj_buf, o_adj, sem.at[3]))
    moves[-1].start()
    for move in moves:
        move.wait()


def on_device(sections, tiles, potential, probe, positions, intensity, fwd_wave, adj_wave, saved_wave):
    n = probe.shape[1]
    nc = n // ROWS
    ticks = intensity.shape[1]
    core, width = potential.shape[1], potential.shape[2]
    margin = (width - core) // 2
    main, ends = (jnp.asarray(x) for x in tables(n))
    held = lambda x: pltpu.VMEM(x.shape, x.dtype)
    vmem = pl.BlockSpec(memory_space=pltpu.VMEM)
    smem = pl.BlockSpec(memory_space=pltpu.SMEM)
    hbm = pl.BlockSpec(memory_space=pltpu.HBM)
    dma = lambda *shape: pltpu.SemaphoreType.DMA(shape)
    wave = lambda count: pltpu.VMEM((count, nc, 2, ROWS, n), BF16)
    lt = pltpu.VMEM((nc, nc, 2 * ROWS, 2 * ROWS), BF16)
    rt = pltpu.VMEM((2 * n, 2 * n), BF16)
    square = pltpu.VMEM((width, width), F32)
    pair = pltpu.VMEM((2, 2, n, n), F32)
    strip = pltpu.VMEM((2, margin, width), BF16)
    wave_next, adj_next, gradient = pl.pallas_call(
        functools.partial(kernel, sections, tiles),
        out_shape=(
            pltpu.VMEM(fwd_wave.shape, BF16),
            pltpu.VMEM(adj_wave.shape, BF16),
            pltpu.VMEM(potential.shape, F32),
        ),
        in_specs=[smem] + [hbm] * 8,
        out_specs=(vmem, vmem, vmem),
        scratch_shapes=[
            wave(ticks + 1), wave(ticks + 1), wave(ticks), wave(ticks),
            held(main), lt, rt, lt, rt,
            pltpu.VMEM((width // LANES, 2 * width, LANES), F32), pair, pair, pltpu.VMEM((2, n, n), F32),
            square, pltpu.VMEM((width // LANES, 4 * width - 2 * n, LANES), F32),
            pltpu.VMEM((nc, 2 * ROWS, n), BF16),
            strip, strip, strip, strip,
            held(potential), held(probe), held(intensity), held(fwd_wave), held(adj_wave),
            held(saved_wave), held(ends), dma(8),
            dma(ticks, nc), dma(ticks, nc), dma(ticks, nc), dma(ticks, nc),
            dma(2), dma(2), dma(2), dma(2),
        ],
        compiler_params=pltpu.CompilerParams(
            collective_id=0, has_side_effects=True, vmem_limit_bytes=VLIM * 1024 * 1024
        ),
        name="window",
    )(jnp.swapaxes(positions, 1, 2), potential, probe, intensity, fwd_wave, adj_wave, saved_wave, main, ends)
    return pl.pallas_call(
        finish,
        out_shape=(
            jax.ShapeDtypeStruct(fwd_wave.shape, F32),
            jax.ShapeDtypeStruct(adj_wave.shape, BF16),
            jax.ShapeDtypeStruct(potential.shape, F32),
        ),
        in_specs=[vmem, vmem, vmem],
        out_specs=(hbm, hbm, hbm),
        scratch_shapes=[pltpu.VMEM(fwd_wave.shape, F32), held(adj_wave), dma(4)],
        name="finish",
    )(wave_next, adj_next, gradient)


def solution(mesh):
    placed = (
        P("depth", "tile", None),
        P(),
        P("tile", None, None),
        P("tile", None, None, None),
        P("depth", "tile", None, None, None),
        P("depth", "tile", None, None, None),
        P("depth", "tile", None, None, None, None),
    )
    return jax.shard_map(
        functools.partial(on_device, mesh.shape["depth"], mesh.shape["tile"]),
        mesh=mesh,
        in_specs=placed,
        out_specs=(
            P("depth", "tile", None, None, None),
            P("depth", "tile", None, None, None),
            P("depth", "tile", None),
        ),
        check_vma=False,
    )
```

```python
import functools
import math

import jax
import jax.numpy as jnp
import numpy as np
from jax import lax
from jax.experimental import pallas as pl
from jax.experimental.pallas import tpu as pltpu
from jax.sharding import PartitionSpec as P

SIGMA = 0.8
DEFOCUS = 6.0
VTOP = 3.0
ROWS = 128
LANES = 128
STEP = 32
VLIM = 40
MESH = pl.DeviceIdType.MESH
F32 = jnp.float32
BF16 = jnp.bfloat16


def rounded(x):
    return x.real.astype(BF16).astype(np.float64) + 1j * x.imag.astype(BF16).astype(np.float64)


def left_blocks(x):
    n = x.shape[0]
    nc = n // ROWS
    out = np.zeros((nc, nc, 2 * ROWS, 2 * ROWS))
    for o in range(nc):
        for c in range(nc):
            b = x[o * ROWS : (o + 1) * ROWS, c * ROWS : (c + 1) * ROWS]
            out[o, c] = np.block([[b.real, -b.imag], [b.imag, b.real]])
    return out.transpose(0, 2, 1, 3).reshape(2 * n, 2 * n)


def right_block(x):
    return np.block([[x.real, x.imag], [-x.imag, x.real]])


def tables(n):
    idx = np.arange(n)
    angle = (idx[:, None] * idx[None, :] % n) * (2.0 * math.pi / n)
    scale = 1.0 / math.sqrt(n)
    cos_t = np.asarray((np.cos(angle) * scale).astype(BF16)).astype(np.float64)
    sin_t = np.asarray((np.sin(angle) * scale).astype(BF16)).astype(np.float64)
    freq = np.where(idx < n // 2, idx, idx - n).astype(np.float64)
    q = np.exp(-1j * math.pi * DEFOCUS * freq * freq / (n * n))
    f = cos_t - 1j * sin_t
    m = (np.conj(f) * q[None, :]) @ f
    m = (m + m.T) / 2
    best = (np.inf, 1.0)
    for size in np.linspace(0.7, 1.4, 64):
        z = (size * np.exp(1j * np.linspace(0.0, math.pi / 2, 128, endpoint=False)))[:, None]
        row = m[0][None, :]
        miss = np.sum(np.abs(rounded(row * z) - row * z) ** 2, axis=1) / size**2
        miss += np.sum(np.abs(rounded(row / z) - row / z) ** 2, axis=1) * size**2
        at = int(np.argmin(miss))
        if miss[at] < best[0]:
            best = (miss[at], z[at, 0])
    z = best[1]
    g = np.conj(f) * q[None, :]
    main = np.stack([left_blocks(z * m), right_block(m / z)]).astype(BF16)
    ends = [p for v in (f, g, g.T) for p in (v.real, v.imag)]
    return main, np.stack(ends).astype(BF16)


def sin_cos(v):
    mid = 0.5 * VTOP * SIGMA
    y = v * SIGMA - mid
    z = y * y
    s = y * (1.0 + z * (-1.0 / 6 + z * (1.0 / 120 + z * (-1.0 / 5040 + z * (1.0 / 362880)))))
    c = 1.0 + z * (-0.5 + z * (1.0 / 24 + z * (-1.0 / 720 + z * (1.0 / 40320))))
    sm, cm = math.sin(mid), math.cos(mid)
    return s * cm + c * sm, c * cm - s * sm


def dot(a, b):
    return jnp.dot(a, b, preferred_element_type=F32)


def kernel(
    sections, tiles,
    pos, pot_h, probe_h, inten_h, fwd_h, adj_h, saved_h, main_h, ends_h,
    o_fwd, o_adj, o_grad,
    in_f, in_b, out_f, out_b, main, l_f, r_f, l_g, r_g,
    cs, tf, ta, bk, total, pad, y_buf,
    halo_out, halo_in, edge_out, edge_in,
    pot, probe, inten, fwd, adj, saved, ends, load_sem,
    send_f, recv_f, send_b, recv_b, send_h, recv_h, send_e, recv_e,
):
    n = probe.shape[1]
    nc = n // ROWS
    cols = n // LANES
    core, width = pot.shape[1], pot.shape[2]
    margin = (width - core) // 2
    ticks = inten.shape[1]
    s = lax.axis_index("depth")
    t = lax.axis_index("tile")
    first, last = s == 0, s == sections - 1
    low, high = t == 0, t == tiles - 1

    loads = {}

    def load(name, src, dst):
        loads[name] = pltpu.make_async_copy(src, dst, load_sem.at[len(loads)])
        return loads[name]

    load("pot", pot_h, pot).start()
    barrier = pltpu.get_barrier_semaphore()
    one = lambda c: jnp.where(c, 1, 0).astype(jnp.int32)

    def greet(cond, axis, to):
        @pl.when(cond)
        def _():
            pl.semaphore_signal(barrier, inc=1, device_id={axis: to}, device_id_type=MESH)

    greet(t > 0, "tile", t - 1)
    greet(t < tiles - 1, "tile", t + 1)
    greet(s > 0, "depth", s - 1)
    greet(s < sections - 1, "depth", s + 1)
    load("main", main_h, main).start()
    load("adj", adj_h, adj).start()
    load("fwd", fwd_h, fwd).start()
    load("probe", probe_h, probe)
    load("ends", ends_h, ends)
    load("inten", inten_h, inten)

    @pl.when(first)
    def _():
        loads["probe"].start()

    @pl.when(last)
    def _():
        loads["ends"].start()
        loads["inten"].start()

    load("saved", saved_h, saved).start()
    loads["pot"].wait()
    halo_out[0] = pot[0, 0:margin, :].astype(BF16)
    halo_out[1] = pot[0, core - margin : core, :].astype(BF16)
    pl.semaphore_wait(barrier, one(s > 0) + one(s < sections - 1) + one(t > 0) + one(t < tiles - 1))

    def hop(src, dst, ssem, rsem, axis, to):
        return pltpu.make_async_remote_copy(
            src_ref=src, dst_ref=dst, send_sem=ssem, recv_sem=rsem,
            device_id={axis: to}, device_id_type=MESH,
        )

    def tile_pair(src, dst, ssem, rsem):
        down = hop(src.at[0], dst.at[1], ssem.at[0], rsem.at[1], "tile", t - 1)
        up = hop(src.at[1], dst.at[0], ssem.at[1], rsem.at[0], "tile", t + 1)
        return down, up

    def tile_start(src, dst, ssem, rsem):
        down, up = tile_pair(src, dst, ssem, rsem)
        pl.when(t > 0)(down.start)
        pl.when(t < tiles - 1)(up.start)

    def tile_wait(src, dst, ssem, rsem):
        down, up = tile_pair(src, dst, ssem, rsem)

        @pl.when(t > 0)
        def _():
            down.wait_send()
            up.wait_recv()

        @pl.when(t < tiles - 1)
        def _():
            up.wait_send()
            down.wait_recv()

    tile_start(halo_out, halo_in, send_h, recv_h)

    def stacked(x):
        return x.reshape(2 * ROWS, n)

    def m_left(o, c):
        return main[0, o * 2 * ROWS : (o + 1) * 2 * ROWS, c * 2 * ROWS : (c + 1) * 2 * ROWS]

    def product(get_left, get_x, r_ref, sink):
        acc = [None] * nc
        for c in range(nc):
            x = get_x(c)
            for o in range(nc):
                term = dot(get_left(o, c), x)
                acc[o] = term if acc[o] is None else acc[o] + term
        for o in range(nc):
            a = acc[o].astype(BF16)
            out = dot(jnp.concatenate([a[0:ROWS, :], a[ROWS : 2 * ROWS, :]], axis=1), r_ref[...])
            sink(o, out[:, 0:n], out[:, n : 2 * n])

    loads["adj"].wait()
    for c in range(nc):
        rows = slice(c * ROWS, (c + 1) * ROWS)
        in_b[0, c, 0] = adj[0, 0, 0, rows, :]
        in_b[0, c, 1] = -adj[0, 0, 1, rows, :]
    loads["main"].wait()

    def keep(o, lur, lui):
        rows = slice(o * ROWS, (o + 1) * ROWS)
        bk[0, rows, :] = lur
        bk[1, rows, :] = lui

    product(m_left, lambda c: stacked(in_b[0, c]), main.at[1], keep)

    def table(src, dst, count):
        for at in range(0, count, STEP):
            sv, cv = sin_cos(src(at))
            for i in range(cols + 1):
                one_tile = slice(i * LANES, (i + 1) * LANES)
                cs[i, pl.ds(2 * (dst + at), STEP, stride=2), :] = cv[:, one_tile]
                cs[i, pl.ds(2 * (dst + at) + 1, STEP, stride=2), :] = sv[:, one_tile]

    table(lambda at: pot[0, at : at + STEP, :], margin, core)
    total[...] = jnp.zeros_like(total)
    spare = width - n
    for i in range(cols + 1):
        pad[i, 0 : 2 * spare, :] = jnp.zeros((2 * spare, LANES), F32)
        pad[i, 2 * (spare + n) :, :] = jnp.zeros((2 * spare, LANES), F32)
    loads["fwd"].wait()
    for c in range(nc):
        rows = slice(c * ROWS, (c + 1) * ROWS)
        for part in range(2):
            in_f[0, c, part] = fwd[0, 0, part, rows, :].astype(BF16)

    @pl.when(first)
    def _():
        loads["probe"].wait()
        for k in range(ticks - 1):
            for c in range(nc):
                for part in range(2):
                    in_f[k + 1, c, part] = probe[part, c * ROWS : (c + 1) * ROWS, :]
        for part in range(2):
            o_fwd[0, 0, part] = probe[part]

    @pl.when(last)
    def _():
        loads["ends"].wait()
        loads["inten"].wait()

        def fill_left(ref, xr, xi):
            for o in range(nc):
                for c in range(nc):
                    br = xr[o * ROWS : (o + 1) * ROWS, c * ROWS : (c + 1) * ROWS]
                    bi = xi[o * ROWS : (o + 1) * ROWS, c * ROWS : (c + 1) * ROWS]
                    ref[o, c, 0:ROWS, 0:ROWS] = br
                    ref[o, c, 0:ROWS, ROWS : 2 * ROWS] = -bi
                    ref[o, c, ROWS : 2 * ROWS, 0:ROWS] = bi
                    ref[o, c, ROWS : 2 * ROWS, ROWS : 2 * ROWS] = br

        def fill_right(ref, xr, xi):
            ref[0:n, 0:n] = xr
            ref[0:n, n : 2 * n] = xi
            ref[n : 2 * n, 0:n] = -xi
            ref[n : 2 * n, n : 2 * n] = xr

        fill_left(l_f, ends[0], ends[1])
        fill_right(r_f, ends[0], ends[1])
        fill_left(l_g, ends[2], ends[3])
        fill_right(r_g, ends[4], ends[5])

    @pl.when(low)
    def _():
        halo_in[0] = jnp.zeros((margin, width), BF16)
        edge_in[0] = jnp.zeros((margin, width), BF16)

    @pl.when(high)
    def _():
        halo_in[1] = jnp.zeros((margin, width), BF16)
        edge_in[1] = jnp.zeros((margin, width), BF16)

    tile_wait(halo_out, halo_in, send_h, recv_h)
    table(lambda at: halo_in[0, at : at + STEP, :].astype(F32), 0, margin)
    table(lambda at: halo_in[1, at : at + STEP, :].astype(F32), margin + core, margin)

    lane = lax.broadcasted_iota(jnp.int32, (STEP, LANES), 1)

    def window(index, out, slot):
        r, c = pos[0, 0, index], pos[0, 1, index]
        turn = lax.rem(LANES - c, LANES)
        own = lane < LANES - c
        for part in range(2):
            for at in range(0, n, STEP):
                rows = pl.ds(2 * (r + at) + part, STEP, stride=2)
                x = [pltpu.roll(cs[i, rows, :], turn, 1) for i in range(cols + 1)]
                for i in range(cols):
                    out[slot, part, at : at + STEP, i * LANES : (i + 1) * LANES] = jnp.where(own, x[i], x[i + 1])

    def windows(k):
        window(k + s, ta, lax.rem(k, 2))
        window(k - s + 2 * sections - 1, tf, lax.rem(k, 2))

    def scatter(k):
        r, c = pos[0, 0, k + s], pos[0, 1, k + s]
        own = lane >= c
        turn = lax.rem(c, LANES)
        for at in range(0, n, STEP):
            rows = slice(at, at + STEP)
            sr = saved[0, 0, k, 0, rows, :].astype(F32)
            si = saved[0, 0, k, 1, rows, :].astype(F32)
            d = (bk[1, rows, :] * sr + bk[0, rows, :] * si) * -SIGMA
            d = [pltpu.roll(d[:, i * LANES : (i + 1) * LANES], turn, 1) for i in range(cols)]
            zero = jnp.zeros((STEP, LANES), F32)
            d = [zero] + d + [zero]
            for i in range(cols + 1):
                pad[i, pl.ds(2 * (spare + at), STEP, stride=2), :] = jnp.where(own, d[i + 1], d[i])
        for at in range(0, width, STEP):
            for i in range(cols + 1):
                total[at : at + STEP, i * LANES : (i + 1) * LANES] += pad[i, pl.ds(2 * (spare - r + at), STEP, stride=2), :]

    def copy_f(k, c):
        return hop(out_f.at[k, c], in_f.at[k + 1, c], send_f.at[k, c], recv_f.at[k, c], "depth", s + 1)

    def copy_b(k, c):
        return hop(out_b.at[k, c], in_b.at[k + 1, c], send_b.at[k, c], recv_b.at[k, c], "depth", s - 1)

    def send_back(k, c, lur, lui):
        rows = slice(c * ROWS, (c + 1) * ROWS)
        slot = lax.rem(k, 2)
        tr, ti = ta[slot, 0, rows, :], ta[slot, 1, rows, :]
        br = tr * lur - ti * lui
        bi = tr * lui + ti * lur
        bk[0, rows, :] = br
        bk[1, rows, :] = bi
        out_b[k, c, 0] = br.astype(BF16)
        out_b[k, c, 1] = bi.astype(BF16)

        @pl.when(jnp.logical_not(first))
        def _():
            copy_b(k, c).start()

    def backward(k):
        def arrived(c):
            @pl.when(jnp.logical_not(last))
            def _():
                copy_b(k - 1, c).wait_recv()
            return stacked(in_b[k, c])

        product(m_left, arrived, main.at[1], functools.partial(send_back, k))

    def entering(k, c, waits):
        if waits:
            @pl.when(jnp.logical_not(first))
            def _():
                copy_f(k - 1, c).wait_recv()
        rows = slice(c * ROWS, (c + 1) * ROWS)
        slot = lax.rem(k, 2)
        wr, wi = in_f[k, c, 0].astype(F32), in_f[k, c, 1].astype(F32)
        tr, ti = tf[slot, 0, rows, :], tf[slot, 1, rows, :]
        return jnp.concatenate([tr * wr - ti * wi, tr * wi + ti * wr], axis=0).astype(BF16)

    def forward(k, waits=True):
        def sink(c, outr, outi):
            out_f[k, c, 0] = outr.astype(BF16)
            out_f[k, c, 1] = outi.astype(BF16)
            copy_f(k, c).start()

        product(m_left, lambda c: entering(k, c, waits), main.at[1], sink)

    def forward_last(k, waits=True):
        def detect(c, vr, vi):
            rows = slice(c * ROWS, (c + 1) * ROWS)
            excess = vr * vr + vi * vi - inten[0, k, rows, :].astype(F32)
            y_buf[c, 0:ROWS, :] = (excess * vr).astype(BF16)
            y_buf[c, ROWS : 2 * ROWS, :] = (excess * vi).astype(BF16)

        def seed(c, outr, outi):
            in_b[k + 1, c, 0] = outr.astype(BF16)
            in_b[k + 1, c, 1] = -outi.astype(BF16)

        product(lambda o, c: l_f[o, c], lambda c: entering(k, c, waits), r_f, detect)
        product(lambda o, c: l_g[o, c], lambda c: y_buf[c], r_g, seed)

    windows(0)
    for c in range(nc):
        rows = slice(c * ROWS, (c + 1) * ROWS)
        send_back(0, c, bk[0, rows, :], bk[1, rows, :])

    @pl.when(jnp.logical_not(last))
    def _():
        forward(0, False)

    @pl.when(last)
    def _():
        forward_last(0, False)

    windows(1)
    loads["saved"].wait()
    scatter(0)

    early = jnp.logical_or(first, jnp.logical_and(lax.rem(s, 2) == 1, jnp.logical_not(last)))

    @pl.when(early)
    def _():
        def tick(k, carry):
            forward(k)

            @pl.when(k < ticks - 1)
            def _():
                windows(k + 1)
            backward(k)
            scatter(k)
            return carry
        lax.fori_loop(1, ticks, tick, 0)

    @pl.when(jnp.logical_not(early))
    def _():
        def tick(k, carry):
            backward(k)
            scatter(k)

            @pl.when(k < ticks - 1)
            def _():
                windows(k + 1)

            @pl.when(jnp.logical_not(last))
            def _():
                forward(k)

            @pl.when(last)
            def _():
                forward_last(k)
            return carry
        lax.fori_loop(1, ticks, tick, 0)

    edge_out[0] = total[0:margin, :].astype(BF16)
    edge_out[1] = total[margin + core :, :].astype(BF16)
    tile_start(edge_out, edge_in, send_e, recv_e)
    o_grad[0, margin : core - margin, :] = total[2 * margin : core, :]
    tile_wait(edge_out, edge_in, send_e, recv_e)
    o_grad[0, 0:margin, :] = total[margin : 2 * margin, :] + edge_in[0].astype(F32)
    o_grad[0, core - margin : core, :] = total[core : core + margin, :] + edge_in[1].astype(F32)
    for c in range(nc):
        rows = slice(c * ROWS, (c + 1) * ROWS)

        @pl.when(jnp.logical_not(last))
        def _():
            copy_b(ticks - 1, c).wait_recv()
        o_adj[0, 0, :, rows, :] = in_b[ticks, c]

        @pl.when(jnp.logical_not(first))
        def _():
            copy_f(ticks - 1, c).wait_recv()
            o_fwd[0, 0, :, rows, :] = in_f[ticks, c]
    for k in range(ticks):
        for c in range(nc):
            @pl.when(jnp.logical_not(last))
            def _():
                copy_f(k, c).wait_send()

            @pl.when(jnp.logical_not(first))
            def _():
                copy_b(k, c).wait_send()


def finish(wave, adj, grad, o_wave, o_adj, o_grad, wave_buf, adj_buf, sem):
    moves = [pltpu.make_async_copy(grad, o_grad, sem.at[0])]
    moves[0].start()
    for part in range(2):
        wave_buf[0, 0, part] = wave[0, 0, part].astype(F32)
        move = pltpu.make_async_copy(wave_buf.at[0, 0, part], o_wave.at[0, 0, part], sem.at[1 + part])
        move.start()
        moves.append(move)
    adj_buf[0, 0, 0] = adj[0, 0, 0]
    adj_buf[0, 0, 1] = -adj[0, 0, 1]
    moves.append(pltpu.make_async_copy(adj_buf, o_adj, sem.at[3]))
    moves[-1].start()
    for move in moves:
        move.wait()


def on_device(sections, tiles, potential, probe, positions, intensity, fwd_wave, adj_wave, saved_wave):
    n = probe.shape[1]
    nc = n // ROWS
    ticks = intensity.shape[1]
    core, width = potential.shape[1], potential.shape[2]
    margin = (width - core) // 2
    main, ends = (jnp.asarray(x) for x in tables(n))
    held = lambda x: pltpu.VMEM(x.shape, x.dtype)
    vmem = pl.BlockSpec(memory_space=pltpu.VMEM)
    smem = pl.BlockSpec(memory_space=pltpu.SMEM)
    hbm = pl.BlockSpec(memory_space=pltpu.HBM)
    dma = lambda *shape: pltpu.SemaphoreType.DMA(shape)
    far = lambda x: pltpu.with_memory_space_constraint(x, pltpu.HBM)
    near = lambda x: pltpu.with_memory_space_constraint(x, pltpu.VMEM)
    wave = lambda count: pltpu.VMEM((count, nc, 2, ROWS, n), BF16)
    lt = pltpu.VMEM((nc, nc, 2 * ROWS, 2 * ROWS), BF16)
    rt = pltpu.VMEM((2 * n, 2 * n), BF16)
    square = pltpu.VMEM((width, width), F32)
    pair = pltpu.VMEM((2, 2, n, n), F32)
    strip = pltpu.VMEM((2, margin, width), BF16)
    wave_next, adj_next, gradient = pl.pallas_call(
        functools.partial(kernel, sections, tiles),
        out_shape=(
            pltpu.VMEM(fwd_wave.shape, BF16),
            pltpu.VMEM(adj_wave.shape, BF16),
            pltpu.VMEM(potential.shape, F32),
        ),
        in_specs=[smem] + [hbm] * 8,
        out_specs=(vmem, vmem, vmem),
        scratch_shapes=[
            wave(ticks + 1), wave(ticks + 1), wave(ticks), wave(ticks),
            held(main), lt, rt, lt, rt,
            pltpu.VMEM((width // LANES, 2 * width, LANES), F32), pair, pair, pltpu.VMEM((2, n, n), F32),
            square, pltpu.VMEM((width // LANES, 4 * width - 2 * n, LANES), F32),
            pltpu.VMEM((nc, 2 * ROWS, n), BF16),
            strip, strip, strip, strip,
            held(potential), held(probe), held(intensity), held(fwd_wave), held(adj_wave),
            held(saved_wave), held(ends), dma(8),
            dma(ticks, nc), dma(ticks, nc), dma(ticks, nc), dma(ticks, nc),
            dma(2), dma(2), dma(2), dma(2),
        ],
        compiler_params=pltpu.CompilerParams(
            collective_id=0, has_side_effects=True, vmem_limit_bytes=VLIM * 1024 * 1024
        ),
        name="window",
    )(
        far(jnp.swapaxes(positions, 1, 2)),
        *(far(x) for x in (potential, probe, intensity, fwd_wave, adj_wave, saved_wave, main, ends)),
    )
    return pl.pallas_call(
        finish,
        out_shape=(
            jax.ShapeDtypeStruct(fwd_wave.shape, F32),
            jax.ShapeDtypeStruct(adj_wave.shape, BF16),
            jax.ShapeDtypeStruct(potential.shape, F32),
        ),
        in_specs=[vmem, vmem, vmem],
        out_specs=(hbm, hbm, hbm),
        scratch_shapes=[pltpu.VMEM(fwd_wave.shape, F32), held(adj_wave), dma(4)],
        name="finish",
    )(near(wave_next), near(adj_next), near(gradient))


def solution(mesh):
    placed = (
        P("depth", "tile", None),
        P(),
        P("tile", None, None),
        P("tile", None, None, None),
        P("depth", "tile", None, None, None),
        P("depth", "tile", None, None, None),
        P("depth", "tile", None, None, None, None),
    )
    return jax.shard_map(
        functools.partial(on_device, mesh.shape["depth"], mesh.shape["tile"]),
        mesh=mesh,
        in_specs=placed,
        out_specs=(
            P("depth", "tile", None, None, None),
            P("depth", "tile", None, None, None),
            P("depth", "tile", None),
        ),
        check_vma=False,
    )
```

```python
import functools
import math

import jax
import jax.numpy as jnp
import numpy as np
from jax import lax
from jax.experimental import pallas as pl
from jax.experimental.pallas import tpu as pltpu
from jax.sharding import PartitionSpec as P

SIGMA = 0.8
DEFOCUS = 6.0
VTOP = 3.0
ROWS = 128
LANES = 128
STEP = 32
VLIM = 40
MESH = pl.DeviceIdType.MESH
F32 = jnp.float32
BF16 = jnp.bfloat16


def rounded(x):
    return x.real.astype(BF16).astype(np.float64) + 1j * x.imag.astype(BF16).astype(np.float64)


def left_blocks(x):
    n = x.shape[0]
    nc = n // ROWS
    out = np.zeros((nc, nc, 2 * ROWS, 2 * ROWS))
    for o in range(nc):
        for c in range(nc):
            b = x[o * ROWS : (o + 1) * ROWS, c * ROWS : (c + 1) * ROWS]
            out[o, c] = np.block([[b.real, -b.imag], [b.imag, b.real]])
    return out.transpose(0, 2, 1, 3).reshape(2 * n, 2 * n)


def right_block(x):
    return np.block([[x.real, x.imag], [-x.imag, x.real]])


def tables(n):
    idx = np.arange(n)
    angle = (idx[:, None] * idx[None, :] % n) * (2.0 * math.pi / n)
    scale = 1.0 / math.sqrt(n)
    cos_t = np.asarray((np.cos(angle) * scale).astype(BF16)).astype(np.float64)
    sin_t = np.asarray((np.sin(angle) * scale).astype(BF16)).astype(np.float64)
    freq = np.where(idx < n // 2, idx, idx - n).astype(np.float64)
    q = np.exp(-1j * math.pi * DEFOCUS * freq * freq / (n * n))
    f = cos_t - 1j * sin_t
    m = (np.conj(f) * q[None, :]) @ f
    m = (m + m.T) / 2
    best = (np.inf, 1.0)
    for size in np.linspace(0.7, 1.4, 64):
        z = (size * np.exp(1j * np.linspace(0.0, math.pi / 2, 128, endpoint=False)))[:, None]
        row = m[0][None, :]
        miss = np.sum(np.abs(rounded(row * z) - row * z) ** 2, axis=1) / size**2
        miss += np.sum(np.abs(rounded(row / z) - row / z) ** 2, axis=1) * size**2
        at = int(np.argmin(miss))
        if miss[at] < best[0]:
            best = (miss[at], z[at, 0])
    z = best[1]
    g = np.conj(f) * q[None, :]
    main = np.stack([left_blocks(z * m), right_block(m / z)]).astype(BF16)
    ends = [p for v in (f, g, g.T) for p in (v.real, v.imag)]
    return main, np.stack(ends).astype(BF16)


def sin_cos(v):
    mid = 0.5 * VTOP * SIGMA
    y = v * SIGMA - mid
    z = y * y
    s = y * (1.0 + z * (-1.0 / 6 + z * (1.0 / 120 + z * (-1.0 / 5040 + z * (1.0 / 362880)))))
    c = 1.0 + z * (-0.5 + z * (1.0 / 24 + z * (-1.0 / 720 + z * (1.0 / 40320))))
    sm, cm = math.sin(mid), math.cos(mid)
    return s * cm + c * sm, c * cm - s * sm


def dot(a, b):
    return jnp.dot(a, b, preferred_element_type=F32)


def kernel(
    sections, tiles,
    pos_h, pot_h, probe_h, inten_h, fwd_h, adj_h, saved_h, main_h, ends_h,
    o_fwd, o_adj, o_grad,
    in_f, in_b, out_f, out_b, main, l_f, r_f, l_g, r_g,
    cs, tf, ta, bk, total, pad, y_buf,
    halo_out, halo_in, edge_out, edge_in,
    pos, pot, probe, inten, fwd, adj, saved, ends, load_sem,
    send_f, recv_f, send_b, recv_b, send_h, recv_h, send_e, recv_e,
):
    n = probe.shape[1]
    nc = n // ROWS
    cols = n // LANES
    core, width = pot.shape[1], pot.shape[2]
    margin = (width - core) // 2
    ticks = inten.shape[1]
    s = lax.axis_index("depth")
    t = lax.axis_index("tile")
    first, last = s == 0, s == sections - 1
    low, high = t == 0, t == tiles - 1

    loads = {}

    def load(name, src, dst):
        loads[name] = pltpu.make_async_copy(src, dst, load_sem.at[len(loads)])
        return loads[name]

    barrier = pltpu.get_barrier_semaphore()
    one = lambda c: jnp.where(c, 1, 0).astype(jnp.int32)

    def greet(cond, axis, to):
        @pl.when(cond)
        def _():
            pl.semaphore_signal(barrier, inc=1, device_id={axis: to}, device_id_type=MESH)

    greet(t > 0, "tile", t - 1)
    greet(t < tiles - 1, "tile", t + 1)
    greet(s > 0, "depth", s - 1)
    greet(s < sections - 1, "depth", s + 1)
    load("pot", pot_h, pot).start()
    load("pos", pos_h, pos).start()
    load("main", main_h, main).start()
    load("adj", adj_h, adj).start()
    load("fwd", fwd_h, fwd).start()
    load("probe", probe_h, probe)
    load("ends", ends_h, ends)
    load("inten", inten_h, inten)

    @pl.when(first)
    def _():
        loads["probe"].start()

    @pl.when(last)
    def _():
        loads["ends"].start()
        loads["inten"].start()

    load("saved", saved_h, saved).start()
    loads["pot"].wait()
    halo_out[0] = pot[0, 0:margin, :].astype(BF16)
    halo_out[1] = pot[0, core - margin : core, :].astype(BF16)
    pl.semaphore_wait(barrier, one(s > 0) + one(s < sections - 1) + one(t > 0) + one(t < tiles - 1))

    def hop(src, dst, ssem, rsem, axis, to):
        return pltpu.make_async_remote_copy(
            src_ref=src, dst_ref=dst, send_sem=ssem, recv_sem=rsem,
            device_id={axis: to}, device_id_type=MESH,
        )

    def tile_pair(src, dst, ssem, rsem):
        down = hop(src.at[0], dst.at[1], ssem.at[0], rsem.at[1], "tile", t - 1)
        up = hop(src.at[1], dst.at[0], ssem.at[1], rsem.at[0], "tile", t + 1)
        return down, up

    def tile_start(src, dst, ssem, rsem):
        down, up = tile_pair(src, dst, ssem, rsem)
        pl.when(t > 0)(down.start)
        pl.when(t < tiles - 1)(up.start)

    def tile_wait(src, dst, ssem, rsem):
        down, up = tile_pair(src, dst, ssem, rsem)

        @pl.when(t > 0)
        def _():
            down.wait_send()
            up.wait_recv()

        @pl.when(t < tiles - 1)
        def _():
            up.wait_send()
            down.wait_recv()

    tile_start(halo_out, halo_in, send_h, recv_h)

    def stacked(x):
        return x.reshape(2 * ROWS, n)

    def m_left(o, c):
        return main[0, o * 2 * ROWS : (o + 1) * 2 * ROWS, c * 2 * ROWS : (c + 1) * 2 * ROWS]

    def product(get_left, get_x, r_ref, sink):
        acc = [None] * nc
        for c in range(nc):
            x = get_x(c)
            for o in range(nc):
                term = dot(get_left(o, c), x)
                acc[o] = term if acc[o] is None else acc[o] + term
        for o in range(nc):
            a = acc[o].astype(BF16)
            out = dot(jnp.concatenate([a[0:ROWS, :], a[ROWS : 2 * ROWS, :]], axis=1), r_ref[...])
            sink(o, out[:, 0:n], out[:, n : 2 * n])

    loads["adj"].wait()
    for c in range(nc):
        rows = slice(c * ROWS, (c + 1) * ROWS)
        in_b[0, c, 0] = adj[0, 0, 0, rows, :]
        in_b[0, c, 1] = -adj[0, 0, 1, rows, :]
    loads["main"].wait()

    def keep(o, lur, lui):
        rows = slice(o * ROWS, (o + 1) * ROWS)
        bk[0, rows, :] = lur
        bk[1, rows, :] = lui

    product(m_left, lambda c: stacked(in_b[0, c]), main.at[1], keep)

    def table(src, dst, count):
        for at in range(0, count, STEP):
            sv, cv = sin_cos(src(at))
            for i in range(cols + 1):
                one_tile = slice(i * LANES, (i + 1) * LANES)
                cs[i, pl.ds(2 * (dst + at), STEP, stride=2), :] = cv[:, one_tile]
                cs[i, pl.ds(2 * (dst + at) + 1, STEP, stride=2), :] = sv[:, one_tile]

    table(lambda at: pot[0, at : at + STEP, :], margin, core)
    total[...] = jnp.zeros_like(total)
    spare = width - n
    for i in range(cols + 1):
        pad[i, 0 : 2 * spare, :] = jnp.zeros((2 * spare, LANES), F32)
        pad[i, 2 * (spare + n) :, :] = jnp.zeros((2 * spare, LANES), F32)
    loads["fwd"].wait()
    for c in range(nc):
        rows = slice(c * ROWS, (c + 1) * ROWS)
        for part in range(2):
            in_f[0, c, part] = fwd[0, 0, part, rows, :].astype(BF16)

    @pl.when(first)
    def _():
        loads["probe"].wait()
        for k in range(ticks - 1):
            for c in range(nc):
                for part in range(2):
                    in_f[k + 1, c, part] = probe[part, c * ROWS : (c + 1) * ROWS, :]
        for part in range(2):
            o_fwd[0, 0, part] = probe[part]

    @pl.when(last)
    def _():
        loads["ends"].wait()
        loads["inten"].wait()

        def fill_left(ref, xr, xi):
            for o in range(nc):
                for c in range(nc):
                    br = xr[o * ROWS : (o + 1) * ROWS, c * ROWS : (c + 1) * ROWS]
                    bi = xi[o * ROWS : (o + 1) * ROWS, c * ROWS : (c + 1) * ROWS]
                    ref[o, c, 0:ROWS, 0:ROWS] = br
                    ref[o, c, 0:ROWS, ROWS : 2 * ROWS] = -bi
                    ref[o, c, ROWS : 2 * ROWS, 0:ROWS] = bi
                    ref[o, c, ROWS : 2 * ROWS, ROWS : 2 * ROWS] = br

        def fill_right(ref, xr, xi):
            ref[0:n, 0:n] = xr
            ref[0:n, n : 2 * n] = xi
            ref[n : 2 * n, 0:n] = -xi
            ref[n : 2 * n, n : 2 * n] = xr

        fill_left(l_f, ends[0], ends[1])
        fill_right(r_f, ends[0], ends[1])
        fill_left(l_g, ends[2], ends[3])
        fill_right(r_g, ends[4], ends[5])

    @pl.when(low)
    def _():
        halo_in[0] = jnp.zeros((margin, width), BF16)
        edge_in[0] = jnp.zeros((margin, width), BF16)

    @pl.when(high)
    def _():
        halo_in[1] = jnp.zeros((margin, width), BF16)
        edge_in[1] = jnp.zeros((margin, width), BF16)

    tile_wait(halo_out, halo_in, send_h, recv_h)
    table(lambda at: halo_in[0, at : at + STEP, :].astype(F32), 0, margin)
    table(lambda at: halo_in[1, at : at + STEP, :].astype(F32), margin + core, margin)

    lane = lax.broadcasted_iota(jnp.int32, (STEP, LANES), 1)

    def window(index, out, slot):
        r, c = pos[0, 0, index], pos[0, 1, index]
        turn = lax.rem(LANES - c, LANES)
        own = lane < LANES - c
        for part in range(2):
            for at in range(0, n, STEP):
                rows = pl.ds(2 * (r + at) + part, STEP, stride=2)
                x = [pltpu.roll(cs[i, rows, :], turn, 1) for i in range(cols + 1)]
                for i in range(cols):
                    out[slot, part, at : at + STEP, i * LANES : (i + 1) * LANES] = jnp.where(own, x[i], x[i + 1])

    def windows(k):
        window(k + s, ta, lax.rem(k, 2))
        window(k - s + 2 * sections - 1, tf, lax.rem(k, 2))

    def scatter(k):
        r, c = pos[0, 0, k + s], pos[0, 1, k + s]
        own = lane >= c
        turn = lax.rem(c, LANES)
        for at in range(0, n, STEP):
            rows = slice(at, at + STEP)
            sr = saved[0, 0, k, 0, rows, :].astype(F32)
            si = saved[0, 0, k, 1, rows, :].astype(F32)
            d = (bk[1, rows, :] * sr + bk[0, rows, :] * si) * -SIGMA
            d = [pltpu.roll(d[:, i * LANES : (i + 1) * LANES], turn, 1) for i in range(cols)]
            zero = jnp.zeros((STEP, LANES), F32)
            d = [zero] + d + [zero]
            for i in range(cols + 1):
                pad[i, pl.ds(2 * (spare + at), STEP, stride=2), :] = jnp.where(own, d[i + 1], d[i])
        for at in range(0, width, STEP):
            for i in range(cols + 1):
                total[at : at + STEP, i * LANES : (i + 1) * LANES] += pad[i, pl.ds(2 * (spare - r + at), STEP, stride=2), :]

    def copy_f(k, c):
        return hop(out_f.at[k, c], in_f.at[k + 1, c], send_f.at[k, c], recv_f.at[k, c], "depth", s + 1)

    def copy_b(k, c):
        return hop(out_b.at[k, c], in_b.at[k + 1, c], send_b.at[k, c], recv_b.at[k, c], "depth", s - 1)

    def send_back(k, c, lur, lui):
        rows = slice(c * ROWS, (c + 1) * ROWS)
        slot = lax.rem(k, 2)
        tr, ti = ta[slot, 0, rows, :], ta[slot, 1, rows, :]
        br = tr * lur - ti * lui
        bi = tr * lui + ti * lur
        bk[0, rows, :] = br
        bk[1, rows, :] = bi
        out_b[k, c, 0] = br.astype(BF16)
        out_b[k, c, 1] = bi.astype(BF16)

        @pl.when(jnp.logical_not(first))
        def _():
            copy_b(k, c).start()

    def backward(k):
        def arrived(c):
            @pl.when(jnp.logical_not(last))
            def _():
                copy_b(k - 1, c).wait_recv()
            return stacked(in_b[k, c])

        product(m_left, arrived, main.at[1], functools.partial(send_back, k))

    def entering(k, c, waits):
        if waits:
            @pl.when(jnp.logical_not(first))
            def _():
                copy_f(k - 1, c).wait_recv()
        rows = slice(c * ROWS, (c + 1) * ROWS)
        slot = lax.rem(k, 2)
        wr, wi = in_f[k, c, 0].astype(F32), in_f[k, c, 1].astype(F32)
        tr, ti = tf[slot, 0, rows, :], tf[slot, 1, rows, :]
        return jnp.concatenate([tr * wr - ti * wi, tr * wi + ti * wr], axis=0).astype(BF16)

    def forward(k, waits=True):
        def sink(c, outr, outi):
            out_f[k, c, 0] = outr.astype(BF16)
            out_f[k, c, 1] = outi.astype(BF16)
            copy_f(k, c).start()

        product(m_left, lambda c: entering(k, c, waits), main.at[1], sink)

    def forward_last(k, waits=True):
        def detect(c, vr, vi):
            rows = slice(c * ROWS, (c + 1) * ROWS)
            excess = vr * vr + vi * vi - inten[0, k, rows, :].astype(F32)
            y_buf[c, 0:ROWS, :] = (excess * vr).astype(BF16)
            y_buf[c, ROWS : 2 * ROWS, :] = (excess * vi).astype(BF16)

        def seed(c, outr, outi):
            in_b[k + 1, c, 0] = outr.astype(BF16)
            in_b[k + 1, c, 1] = -outi.astype(BF16)

        product(lambda o, c: l_f[o, c], lambda c: entering(k, c, waits), r_f, detect)
        product(lambda o, c: l_g[o, c], lambda c: y_buf[c], r_g, seed)

    loads["pos"].wait()
    windows(0)
    for c in range(nc):
        rows = slice(c * ROWS, (c + 1) * ROWS)
        send_back(0, c, bk[0, rows, :], bk[1, rows, :])

    @pl.when(jnp.logical_not(last))
    def _():
        forward(0, False)

    @pl.when(last)
    def _():
        forward_last(0, False)

    windows(1)
    loads["saved"].wait()
    scatter(0)

    early = jnp.logical_or(first, jnp.logical_and(lax.rem(s, 2) == 1, jnp.logical_not(last)))

    @pl.when(early)
    def _():
        def tick(k, carry):
            forward(k)

            @pl.when(k < ticks - 1)
            def _():
                windows(k + 1)
            backward(k)
            scatter(k)
            return carry
        lax.fori_loop(1, ticks, tick, 0)

    @pl.when(jnp.logical_not(early))
    def _():
        def tick(k, carry):
            backward(k)
            scatter(k)

            @pl.when(k < ticks - 1)
            def _():
                windows(k + 1)

            @pl.when(jnp.logical_not(last))
            def _():
                forward(k)

            @pl.when(last)
            def _():
                forward_last(k)
            return carry
        lax.fori_loop(1, ticks, tick, 0)

    edge_out[0] = total[0:margin, :].astype(BF16)
    edge_out[1] = total[margin + core :, :].astype(BF16)
    tile_start(edge_out, edge_in, send_e, recv_e)
    o_grad[0, margin : core - margin, :] = total[2 * margin : core, :]
    tile_wait(edge_out, edge_in, send_e, recv_e)
    o_grad[0, 0:margin, :] = total[margin : 2 * margin, :] + edge_in[0].astype(F32)
    o_grad[0, core - margin : core, :] = total[core : core + margin, :] + edge_in[1].astype(F32)
    for c in range(nc):
        rows = slice(c * ROWS, (c + 1) * ROWS)

        @pl.when(jnp.logical_not(last))
        def _():
            copy_b(ticks - 1, c).wait_recv()
        o_adj[0, 0, :, rows, :] = in_b[ticks, c]

        @pl.when(jnp.logical_not(first))
        def _():
            copy_f(ticks - 1, c).wait_recv()
            o_fwd[0, 0, :, rows, :] = in_f[ticks, c]
    for k in range(ticks):
        for c in range(nc):
            @pl.when(jnp.logical_not(last))
            def _():
                copy_f(k, c).wait_send()

            @pl.when(jnp.logical_not(first))
            def _():
                copy_b(k, c).wait_send()


def finish(wave, adj, grad, o_wave, o_adj, o_grad, wave_buf, adj_buf, sem):
    moves = [pltpu.make_async_copy(grad, o_grad, sem.at[0])]
    moves[0].start()
    for part in range(2):
        wave_buf[0, 0, part] = wave[0, 0, part].astype(F32)
        move = pltpu.make_async_copy(wave_buf.at[0, 0, part], o_wave.at[0, 0, part], sem.at[1 + part])
        move.start()
        moves.append(move)
    adj_buf[0, 0, 0] = adj[0, 0, 0]
    adj_buf[0, 0, 1] = -adj[0, 0, 1]
    moves.append(pltpu.make_async_copy(adj_buf, o_adj, sem.at[3]))
    moves[-1].start()
    for move in moves:
        move.wait()


def on_device(sections, tiles, potential, probe, positions, intensity, fwd_wave, adj_wave, saved_wave):
    n = probe.shape[1]
    nc = n // ROWS
    ticks = intensity.shape[1]
    core, width = potential.shape[1], potential.shape[2]
    margin = (width - core) // 2
    main, ends = (jnp.asarray(x) for x in tables(n))
    held = lambda x: pltpu.VMEM(x.shape, x.dtype)
    vmem = pl.BlockSpec(memory_space=pltpu.VMEM)
    spots = jnp.swapaxes(positions, 1, 2)
    hbm = pl.BlockSpec(memory_space=pltpu.HBM)
    dma = lambda *shape: pltpu.SemaphoreType.DMA(shape)
    far = lambda x: pltpu.with_memory_space_constraint(x, pltpu.HBM)
    near = lambda x: pltpu.with_memory_space_constraint(x, pltpu.VMEM)
    wave = lambda count: pltpu.VMEM((count, nc, 2, ROWS, n), BF16)
    lt = pltpu.VMEM((nc, nc, 2 * ROWS, 2 * ROWS), BF16)
    rt = pltpu.VMEM((2 * n, 2 * n), BF16)
    square = pltpu.VMEM((width, width), F32)
    pair = pltpu.VMEM((2, 2, n, n), F32)
    strip = pltpu.VMEM((2, margin, width), BF16)
    wave_next, adj_next, gradient = pl.pallas_call(
        functools.partial(kernel, sections, tiles),
        out_shape=(
            pltpu.VMEM(fwd_wave.shape, BF16),
            pltpu.VMEM(adj_wave.shape, BF16),
            pltpu.VMEM(potential.shape, F32),
        ),
        in_specs=[hbm] * 9,
        out_specs=(vmem, vmem, vmem),
        scratch_shapes=[
            wave(ticks + 1), wave(ticks + 1), wave(ticks), wave(ticks),
            held(main), lt, rt, lt, rt,
            pltpu.VMEM((width // LANES, 2 * width, LANES), F32), pair, pair, pltpu.VMEM((2, n, n), F32),
            square, pltpu.VMEM((width // LANES, 4 * width - 2 * n, LANES), F32),
            pltpu.VMEM((nc, 2 * ROWS, n), BF16),
            strip, strip, strip, strip,
            pltpu.SMEM(spots.shape, spots.dtype), held(potential), held(probe), held(intensity), held(fwd_wave), held(adj_wave),
            held(saved_wave), held(ends), dma(9),
            dma(ticks, nc), dma(ticks, nc), dma(ticks, nc), dma(ticks, nc),
            dma(2), dma(2), dma(2), dma(2),
        ],
        compiler_params=pltpu.CompilerParams(
            collective_id=0, has_side_effects=True, vmem_limit_bytes=VLIM * 1024 * 1024
        ),
        name="window",
    )(
        *(far(x) for x in (spots, potential, probe, intensity, fwd_wave, adj_wave, saved_wave, main, ends)),
    )
    return pl.pallas_call(
        finish,
        out_shape=(
            jax.ShapeDtypeStruct(fwd_wave.shape, F32),
            jax.ShapeDtypeStruct(adj_wave.shape, BF16),
            jax.ShapeDtypeStruct(potential.shape, F32),
        ),
        in_specs=[vmem, vmem, vmem],
        out_specs=(hbm, hbm, hbm),
        scratch_shapes=[pltpu.VMEM(fwd_wave.shape, F32), held(adj_wave), dma(4)],
        name="finish",
    )(near(wave_next), near(adj_next), near(gradient))


def solution(mesh):
    placed = (
        P("depth", "tile", None),
        P(),
        P("tile", None, None),
        P("tile", None, None, None),
        P("depth", "tile", None, None, None),
        P("depth", "tile", None, None, None),
        P("depth", "tile", None, None, None, None),
    )
    return jax.shard_map(
        functools.partial(on_device, mesh.shape["depth"], mesh.shape["tile"]),
        mesh=mesh,
        in_specs=placed,
        out_specs=(
            P("depth", "tile", None, None, None),
            P("depth", "tile", None, None, None),
            P("depth", "tile", None),
        ),
        check_vma=False,
    )
```

```python
import functools
import math

import jax
import jax.numpy as jnp
import numpy as np
from jax import lax
from jax.experimental import pallas as pl
from jax.experimental.pallas import tpu as pltpu
from jax.sharding import PartitionSpec as P

SIGMA = 0.8
DEFOCUS = 6.0
VTOP = 3.0
ROWS = 128
LANES = 128
STEP = 32
VLIM = 40
MESH = pl.DeviceIdType.MESH
F32 = jnp.float32
BF16 = jnp.bfloat16


def rounded(x):
    return x.real.astype(BF16).astype(np.float64) + 1j * x.imag.astype(BF16).astype(np.float64)


def left_blocks(x):
    n = x.shape[0]
    nc = n // ROWS
    out = np.zeros((nc, nc, 2 * ROWS, 2 * ROWS))
    for o in range(nc):
        for c in range(nc):
            b = x[o * ROWS : (o + 1) * ROWS, c * ROWS : (c + 1) * ROWS]
            out[o, c] = np.block([[b.real, -b.imag], [b.imag, b.real]])
    return out.transpose(0, 2, 1, 3).reshape(2 * n, 2 * n)


def right_block(x):
    return np.block([[x.real, x.imag], [-x.imag, x.real]])


def tables(n):
    idx = np.arange(n)
    angle = (idx[:, None] * idx[None, :] % n) * (2.0 * math.pi / n)
    scale = 1.0 / math.sqrt(n)
    cos_t = np.asarray((np.cos(angle) * scale).astype(BF16)).astype(np.float64)
    sin_t = np.asarray((np.sin(angle) * scale).astype(BF16)).astype(np.float64)
    freq = np.where(idx < n // 2, idx, idx - n).astype(np.float64)
    q = np.exp(-1j * math.pi * DEFOCUS * freq * freq / (n * n))
    f = cos_t - 1j * sin_t
    m = (np.conj(f) * q[None, :]) @ f
    m = (m + m.T) / 2
    best = (np.inf, 1.0)
    for size in np.linspace(0.7, 1.4, 64):
        z = (size * np.exp(1j * np.linspace(0.0, math.pi / 2, 128, endpoint=False)))[:, None]
        row = m[0][None, :]
        miss = np.sum(np.abs(rounded(row * z) - row * z) ** 2, axis=1) / size**2
        miss += np.sum(np.abs(rounded(row / z) - row / z) ** 2, axis=1) * size**2
        at = int(np.argmin(miss))
        if miss[at] < best[0]:
            best = (miss[at], z[at, 0])
    z = best[1]
    g = np.conj(f) * q[None, :]
    main = np.stack([left_blocks(z * m), right_block(m / z)]).astype(BF16)
    ends = [p for v in (f, g, g.T) for p in (v.real, v.imag)]
    return main, np.stack(ends).astype(BF16)


def sin_cos(v):
    mid = 0.5 * VTOP * SIGMA
    y = v * SIGMA - mid
    z = y * y
    s = y * (1.0 + z * (-1.0 / 6 + z * (1.0 / 120 + z * (-1.0 / 5040 + z * (1.0 / 362880)))))
    c = 1.0 + z * (-0.5 + z * (1.0 / 24 + z * (-1.0 / 720 + z * (1.0 / 40320))))
    sm, cm = math.sin(mid), math.cos(mid)
    return s * cm + c * sm, c * cm - s * sm


def dot(a, b):
    return jnp.dot(a, b, preferred_element_type=F32)


def kernel(
    sections, tiles,
    pos_h, pot_h, probe_h, inten_h, fwd_h, adj_h, saved_h, main_h, ends_h,
    o_fwd, o_adj, o_grad,
    in_f, in_b, out_f, out_b, main, l_f, r_f, l_g, r_g,
    cs, tf, ta, bk, total, pad, y_buf,
    halo_out, halo_in, edge_out, edge_in, view_out, view_in,
    pos, pot, probe, inten, fwd, adj, saved, ends, load_sem,
    send_f, recv_f, send_b, recv_b, send_h, recv_h, send_e, recv_e, send_v, recv_v, ready,
):
    n = probe.shape[1]
    nc = n // ROWS
    cols = n // LANES
    core, width = pot.shape[1], pot.shape[2]
    margin = (width - core) // 2
    ticks = inten.shape[1]
    s = lax.axis_index("depth")
    t = lax.axis_index("tile")
    first, last = s == 0, s == sections - 1
    low, high = t == 0, t == tiles - 1
    ahead = jnp.logical_and(lax.rem(s, 2) == 0, s > 0)
    behind = jnp.logical_and(lax.rem(s, 2) == 1, s < sections - 1)

    loads = {}

    def load(name, src, dst):
        loads[name] = pltpu.make_async_copy(src, dst, load_sem.at[len(loads)])
        return loads[name]

    barrier = pltpu.get_barrier_semaphore()
    one = lambda c: jnp.where(c, 1, 0).astype(jnp.int32)

    def greet(cond, axis, to):
        @pl.when(cond)
        def _():
            pl.semaphore_signal(barrier, inc=1, device_id={axis: to}, device_id_type=MESH)

    greet(t > 0, "tile", t - 1)
    greet(t < tiles - 1, "tile", t + 1)
    greet(s < sections - 1, "depth", s + 1)
    load("pot", pot_h, pot).start()
    load("pos", pos_h, pos).start()
    load("main", main_h, main).start()
    load("adj", adj_h, adj).start()
    load("fwd", fwd_h, fwd).start()
    load("probe", probe_h, probe)
    load("ends", ends_h, ends)
    load("inten", inten_h, inten)

    @pl.when(first)
    def _():
        loads["probe"].start()

    @pl.when(last)
    def _():
        loads["ends"].start()
        loads["inten"].start()

    load("saved", saved_h, saved).start()
    loads["pot"].wait()
    halo_out[0] = pot[0, 0:margin, :].astype(BF16)
    halo_out[1] = pot[0, core - margin : core, :].astype(BF16)
    pl.semaphore_wait(barrier, one(s > 0) + one(t > 0) + one(t < tiles - 1))

    def hop(src, dst, ssem, rsem, axis, to):
        return pltpu.make_async_remote_copy(
            src_ref=src, dst_ref=dst, send_sem=ssem, recv_sem=rsem,
            device_id={axis: to}, device_id_type=MESH,
        )

    def tile_pair(src, dst, ssem, rsem):
        down = hop(src.at[0], dst.at[1], ssem.at[0], rsem.at[1], "tile", t - 1)
        up = hop(src.at[1], dst.at[0], ssem.at[1], rsem.at[0], "tile", t + 1)
        return down, up

    def tile_start(src, dst, ssem, rsem):
        down, up = tile_pair(src, dst, ssem, rsem)
        pl.when(t > 0)(down.start)
        pl.when(t < tiles - 1)(up.start)

    def tile_wait(src, dst, ssem, rsem):
        down, up = tile_pair(src, dst, ssem, rsem)

        @pl.when(t > 0)
        def _():
            down.wait_send()
            up.wait_recv()

        @pl.when(t < tiles - 1)
        def _():
            up.wait_send()
            down.wait_recv()

    tile_start(halo_out, halo_in, send_h, recv_h)

    @pl.when(s > 0)
    def _():
        pl.semaphore_signal(ready, inc=1, device_id={"depth": s - 1}, device_id_type=MESH)

    def stacked(x):
        return x.reshape(2 * ROWS, n)

    def m_left(o, c):
        return main[0, o * 2 * ROWS : (o + 1) * 2 * ROWS, c * 2 * ROWS : (c + 1) * 2 * ROWS]

    def product(get_left, get_x, r_ref, sink):
        acc = [None] * nc
        for c in range(nc):
            x = get_x(c)
            for o in range(nc):
                term = dot(get_left(o, c), x)
                acc[o] = term if acc[o] is None else acc[o] + term
        for o in range(nc):
            a = acc[o].astype(BF16)
            out = dot(jnp.concatenate([a[0:ROWS, :], a[ROWS : 2 * ROWS, :]], axis=1), r_ref[...])
            sink(o, out[:, 0:n], out[:, n : 2 * n])

    def copy_f(k, c):
        return hop(out_f.at[k, c], in_f.at[k + 1, c], send_f.at[k, c], recv_f.at[k, c], "depth", s + 1)

    def copy_b(k, c):
        return hop(out_b.at[k, c], in_b.at[k + 1, c], send_b.at[k, c], recv_b.at[k, c], "depth", s - 1)

    def last_f(c):
        k, rows = ticks - 1, slice(c * ROWS, (c + 1) * ROWS)
        return hop(out_f.at[k, c], o_fwd.at[0, 0, :, rows, :], send_f.at[k, c], recv_f.at[k, c], "depth", s + 1)

    def last_b(c):
        k, rows = ticks - 1, slice(c * ROWS, (c + 1) * ROWS)
        return hop(out_b.at[k, c], o_adj.at[0, 0, :, rows, :], send_b.at[k, c], recv_b.at[k, c], "depth", s - 1)

    def launch(k, c, copy, final):
        if isinstance(k, int):
            copy(k, c).start()
        else:
            pl.when(k < ticks - 1)(lambda: copy(k, c).start())
            pl.when(k == ticks - 1)(lambda: final(c).start())

    loads["adj"].wait()
    for c in range(nc):
        rows = slice(c * ROWS, (c + 1) * ROWS)
        in_b[0, c, 0] = adj[0, 0, 0, rows, :]
        in_b[0, c, 1] = -adj[0, 0, 1, rows, :]
    loads["main"].wait()

    def keep(o, lur, lui):
        rows = slice(o * ROWS, (o + 1) * ROWS)
        bk[0, rows, :] = lur
        bk[1, rows, :] = lui
        out_b[0, o, 0] = lur.astype(BF16)
        out_b[0, o, 1] = lui.astype(BF16)
        pl.when(ahead)(lambda: copy_b(0, o).start())

    product(m_left, lambda c: stacked(in_b[0, c]), main.at[1], keep)

    def table(src, dst, count):
        for at in range(0, count, STEP):
            v = src(at)
            sv, cv = sin_cos(v)
            for i in range(cols + 1):
                one_tile = slice(i * LANES, (i + 1) * LANES)
                for part, part_v in enumerate((cv, sv, v)):
                    cs[i, pl.ds(3 * (dst + at) + part, STEP, stride=3), :] = part_v[:, one_tile]

    table(lambda at: pot[0, at : at + STEP, :], margin, core)
    total[...] = jnp.zeros_like(total)
    spare = width - n
    for i in range(cols + 1):
        pad[i, 0 : 2 * spare, :] = jnp.zeros((2 * spare, LANES), F32)
        pad[i, 2 * (spare + n) :, :] = jnp.zeros((2 * spare, LANES), F32)
    loads["fwd"].wait()
    for c in range(nc):
        rows = slice(c * ROWS, (c + 1) * ROWS)
        for part in range(2):
            in_f[0, c, part] = fwd[0, 0, part, rows, :].astype(BF16)

    @pl.when(first)
    def _():
        loads["probe"].wait()
        for k in range(ticks - 1):
            for c in range(nc):
                for part in range(2):
                    in_f[k + 1, c, part] = probe[part, c * ROWS : (c + 1) * ROWS, :]
        for part in range(2):
            o_fwd[0, 0, part] = probe[part]

    @pl.when(last)
    def _():
        loads["ends"].wait()
        loads["inten"].wait()

        def fill_left(ref, xr, xi):
            for o in range(nc):
                for c in range(nc):
                    br = xr[o * ROWS : (o + 1) * ROWS, c * ROWS : (c + 1) * ROWS]
                    bi = xi[o * ROWS : (o + 1) * ROWS, c * ROWS : (c + 1) * ROWS]
                    ref[o, c, 0:ROWS, 0:ROWS] = br
                    ref[o, c, 0:ROWS, ROWS : 2 * ROWS] = -bi
                    ref[o, c, ROWS : 2 * ROWS, 0:ROWS] = bi
                    ref[o, c, ROWS : 2 * ROWS, ROWS : 2 * ROWS] = br

        def fill_right(ref, xr, xi):
            ref[0:n, 0:n] = xr
            ref[0:n, n : 2 * n] = xi
            ref[n : 2 * n, 0:n] = -xi
            ref[n : 2 * n, n : 2 * n] = xr

        fill_left(l_f, ends[0], ends[1])
        fill_right(r_f, ends[0], ends[1])
        fill_left(l_g, ends[2], ends[3])
        fill_right(r_g, ends[4], ends[5])

    @pl.when(low)
    def _():
        halo_in[0] = jnp.zeros((margin, width), BF16)
        edge_in[0] = jnp.zeros((margin, width), BF16)

    @pl.when(high)
    def _():
        halo_in[1] = jnp.zeros((margin, width), BF16)
        edge_in[1] = jnp.zeros((margin, width), BF16)

    tile_wait(halo_out, halo_in, send_h, recv_h)
    table(lambda at: halo_in[0, at : at + STEP, :].astype(F32), 0, margin)
    table(lambda at: halo_in[1, at : at + STEP, :].astype(F32), margin + core, margin)

    lane = lax.broadcasted_iota(jnp.int32, (STEP, LANES), 1)

    def window(index, parts, store):
        r, c = pos[0, 0, index], pos[0, 1, index]
        turn = lax.rem(LANES - c, LANES)
        own = lane < LANES - c
        for part in parts:
            for at in range(0, n, STEP):
                rows = pl.ds(3 * (r + at) + part, STEP, stride=3)
                x = [pltpu.roll(cs[i, rows, :], turn, 1) for i in range(cols + 1)]
                for i in range(cols):
                    store(part, at, slice(i * LANES, (i + 1) * LANES), jnp.where(own, x[i], x[i + 1]))

    def window_b(k):
        def store(part, at, tile, x):
            ta[lax.rem(k, 2), part, at : at + STEP, tile] = x
        window(k + s, range(2), store)

    def window_f(k):
        def store(part, at, tile, x):
            tf[lax.rem(k, 2), part, at : at + STEP, tile] = x
        window(k - s + 2 * sections - 1, range(2), store)

    def copy_v(c):
        return hop(view_out.at[c], view_in.at[c], send_v.at[c], recv_v.at[c], "depth", s - 1)

    def send_view():
        def store(part, at, tile, x):
            view_out[at // ROWS, at % ROWS : at % ROWS + STEP, tile] = x.astype(BF16)
        window(s, (2,), store)
        for c in range(nc):
            copy_v(c).start()

    def windows(k):
        window_b(k)
        window_f(k)

    def scatter(k):
        r, c = pos[0, 0, k + s], pos[0, 1, k + s]
        own = lane >= c
        turn = lax.rem(c, LANES)
        for at in range(0, n, STEP):
            rows = slice(at, at + STEP)
            sr = saved[0, 0, k, 0, rows, :].astype(F32)
            si = saved[0, 0, k, 1, rows, :].astype(F32)
            d = (bk[1, rows, :] * sr + bk[0, rows, :] * si) * -SIGMA
            d = [pltpu.roll(d[:, i * LANES : (i + 1) * LANES], turn, 1) for i in range(cols)]
            zero = jnp.zeros((STEP, LANES), F32)
            d = [zero] + d + [zero]
            for i in range(cols + 1):
                pad[i, pl.ds(2 * (spare + at), STEP, stride=2), :] = jnp.where(own, d[i + 1], d[i])

        def add(lo, hi):
            for at in range(lo, hi, STEP):
                for i in range(cols + 1):
                    total[at : at + STEP, i * LANES : (i + 1) * LANES] += pad[
                        i, pl.ds(2 * (spare - r + at), STEP, stride=2), :
                    ]

        add(0, margin)
        add(margin + core, width)
        if not isinstance(k, int):
            @pl.when(k == ticks - 1)
            def _():
                edge_out[0] = total[0:margin, :].astype(BF16)
                edge_out[1] = total[margin + core :, :].astype(BF16)
                tile_start(edge_out, edge_in, send_e, recv_e)
        add(margin, margin + core)

    def send_back(k, c, lur, lui):
        rows = slice(c * ROWS, (c + 1) * ROWS)
        slot = lax.rem(k, 2)
        tr, ti = ta[slot, 0, rows, :], ta[slot, 1, rows, :]
        br = tr * lur - ti * lui
        bi = tr * lui + ti * lur
        bk[0, rows, :] = br
        bk[1, rows, :] = bi

        sends = jnp.logical_not(first)
        if isinstance(k, int):
            sends = jnp.logical_and(sends, jnp.logical_not(ahead))

        @pl.when(sends)
        def _():
            out_b[k, c, 0] = br.astype(BF16)
            out_b[k, c, 1] = bi.astype(BF16)
            launch(k, c, copy_b, last_b)

    def backward(k, bare=False):
        def arrived(c):
            @pl.when(jnp.logical_not(last))
            def _():
                copy_b(k - 1, c).wait_recv()
            if bare:
                @pl.when(jnp.logical_and(k == 1, behind))
                def _():
                    copy_v(c).wait_recv()
                    lur, lui = in_b[1, c, 0].astype(F32), in_b[1, c, 1].astype(F32)
                    ti, tr = sin_cos(view_in[c].astype(F32))
                    in_b[1, c, 0] = (tr * lur - ti * lui).astype(BF16)
                    in_b[1, c, 1] = (tr * lui + ti * lur).astype(BF16)
            return stacked(in_b[k, c])

        product(m_left, arrived, main.at[1], functools.partial(send_back, k))

    def entering(k, c, waits):
        if waits:
            @pl.when(jnp.logical_not(first))
            def _():
                copy_f(k - 1, c).wait_recv()
        rows = slice(c * ROWS, (c + 1) * ROWS)
        slot = lax.rem(k, 2)
        wr, wi = in_f[k, c, 0].astype(F32), in_f[k, c, 1].astype(F32)
        tr, ti = tf[slot, 0, rows, :], tf[slot, 1, rows, :]
        return jnp.concatenate([tr * wr - ti * wi, tr * wi + ti * wr], axis=0).astype(BF16)

    def forward(k, waits=True):
        def sink(c, outr, outi):
            out_f[k, c, 0] = outr.astype(BF16)
            out_f[k, c, 1] = outi.astype(BF16)
            launch(k, c, copy_f, last_f)

        product(m_left, lambda c: entering(k, c, waits), main.at[1], sink)

    def forward_last(k, waits=True):
        def detect(c, vr, vi):
            rows = slice(c * ROWS, (c + 1) * ROWS)
            excess = vr * vr + vi * vi - inten[0, k, rows, :].astype(F32)
            y_buf[c, 0:ROWS, :] = (excess * vr).astype(BF16)
            y_buf[c, ROWS : 2 * ROWS, :] = (excess * vi).astype(BF16)

        def seed(c, outr, outi):
            in_b[k + 1, c, 0] = outr.astype(BF16)
            in_b[k + 1, c, 1] = -outi.astype(BF16)

        product(lambda o, c: l_f[o, c], lambda c: entering(k, c, waits), r_f, detect)
        product(lambda o, c: l_g[o, c], lambda c: y_buf[c], r_g, seed)

    loads["pos"].wait()
    pl.when(ahead)(send_view)
    window_b(0)
    for c in range(nc):
        rows = slice(c * ROWS, (c + 1) * ROWS)
        send_back(0, c, bk[0, rows, :], bk[1, rows, :])
    window_f(0)

    @pl.when(jnp.logical_not(last))
    def _():
        pl.semaphore_wait(ready, 1)
        forward(0, False)

    @pl.when(last)
    def _():
        forward_last(0, False)

    windows(1)
    loads["saved"].wait()
    scatter(0)

    early = jnp.logical_or(first, jnp.logical_and(lax.rem(s, 2) == 1, jnp.logical_not(last)))

    @pl.when(early)
    def _():
        def tick(k, carry):
            forward(k)

            @pl.when(k < ticks - 1)
            def _():
                windows(k + 1)
            backward(k, True)
            scatter(k)
            return carry
        lax.fori_loop(1, ticks, tick, 0)

    @pl.when(jnp.logical_not(early))
    def _():
        def tick(k, carry):
            backward(k)
            scatter(k)

            @pl.when(k < ticks - 1)
            def _():
                windows(k + 1)

            @pl.when(jnp.logical_not(last))
            def _():
                forward(k)

            @pl.when(last)
            def _():
                forward_last(k)
            return carry
        lax.fori_loop(1, ticks, tick, 0)

    o_grad[0, margin : core - margin, :] = total[2 * margin : core, :]
    tile_wait(edge_out, edge_in, send_e, recv_e)
    o_grad[0, 0:margin, :] = total[margin : 2 * margin, :] + edge_in[0].astype(F32)
    o_grad[0, core - margin : core, :] = total[core : core + margin, :] + edge_in[1].astype(F32)
    @pl.when(last)
    def _():
        for c in range(nc):
            o_adj[0, 0, :, c * ROWS : (c + 1) * ROWS, :] = in_b[ticks, c]

    for c in range(nc):
        @pl.when(jnp.logical_not(last))
        def _():
            last_b(c).wait_recv()

        @pl.when(jnp.logical_not(first))
        def _():
            last_f(c).wait_recv()
    for c in range(nc):
        pl.when(ahead)(lambda: copy_v(c).wait_send())
    for k in range(ticks):
        for c in range(nc):
            @pl.when(jnp.logical_not(last))
            def _():
                copy_f(k, c).wait_send()

            @pl.when(jnp.logical_not(first))
            def _():
                copy_b(k, c).wait_send()


def finish(wave, adj, grad, o_wave, o_adj, o_grad, wave_buf, adj_buf, sem):
    moves = [pltpu.make_async_copy(grad, o_grad, sem.at[0])]
    moves[0].start()
    for part in range(2):
        wave_buf[0, 0, part] = wave[0, 0, part].astype(F32)
        move = pltpu.make_async_copy(wave_buf.at[0, 0, part], o_wave.at[0, 0, part], sem.at[1 + part])
        move.start()
        moves.append(move)
    adj_buf[0, 0, 0] = adj[0, 0, 0]
    adj_buf[0, 0, 1] = -adj[0, 0, 1]
    moves.append(pltpu.make_async_copy(adj_buf, o_adj, sem.at[3]))
    moves[-1].start()
    for move in moves:
        move.wait()


def on_device(sections, tiles, potential, probe, positions, intensity, fwd_wave, adj_wave, saved_wave):
    n = probe.shape[1]
    nc = n // ROWS
    ticks = intensity.shape[1]
    core, width = potential.shape[1], potential.shape[2]
    margin = (width - core) // 2
    main, ends = (jnp.asarray(x) for x in tables(n))
    held = lambda x: pltpu.VMEM(x.shape, x.dtype)
    vmem = pl.BlockSpec(memory_space=pltpu.VMEM)
    spots = jnp.swapaxes(positions, 1, 2)
    hbm = pl.BlockSpec(memory_space=pltpu.HBM)
    dma = lambda *shape: pltpu.SemaphoreType.DMA(shape)
    far = lambda x: pltpu.with_memory_space_constraint(x, pltpu.HBM)
    near = lambda x: pltpu.with_memory_space_constraint(x, pltpu.VMEM)
    wave = lambda count: pltpu.VMEM((count, nc, 2, ROWS, n), BF16)
    lt = pltpu.VMEM((nc, nc, 2 * ROWS, 2 * ROWS), BF16)
    rt = pltpu.VMEM((2 * n, 2 * n), BF16)
    square = pltpu.VMEM((width, width), F32)
    pair = pltpu.VMEM((2, 2, n, n), F32)
    strip = pltpu.VMEM((2, margin, width), BF16)
    wave_next, adj_next, gradient = pl.pallas_call(
        functools.partial(kernel, sections, tiles),
        out_shape=(
            pltpu.VMEM(fwd_wave.shape, BF16),
            pltpu.VMEM(adj_wave.shape, BF16),
            pltpu.VMEM(potential.shape, F32),
        ),
        in_specs=[hbm] * 9,
        out_specs=(vmem, vmem, vmem),
        scratch_shapes=[
            wave(ticks + 1), wave(ticks + 1), wave(ticks), wave(ticks),
            held(main), lt, rt, lt, rt,
            pltpu.VMEM((width // LANES, 3 * width, LANES), F32), pair, pair, pltpu.VMEM((2, n, n), F32),
            square, pltpu.VMEM((width // LANES, 4 * width - 2 * n, LANES), F32),
            pltpu.VMEM((nc, 2 * ROWS, n), BF16),
            strip, strip, strip, strip, pltpu.VMEM((nc, ROWS, n), BF16), pltpu.VMEM((nc, ROWS, n), BF16),
            pltpu.SMEM(spots.shape, spots.dtype), held(potential), held(probe), held(intensity), held(fwd_wave), held(adj_wave),
            held(saved_wave), held(ends), dma(9),
            dma(ticks, nc), dma(ticks, nc), dma(ticks, nc), dma(ticks, nc),
            dma(2), dma(2), dma(2), dma(2), dma(nc), dma(nc), pltpu.SemaphoreType.REGULAR,
        ],
        compiler_params=pltpu.CompilerParams(
            collective_id=0, has_side_effects=True, vmem_limit_bytes=VLIM * 1024 * 1024
        ),
        name="window",
    )(
        *(far(x) for x in (spots, potential, probe, intensity, fwd_wave, adj_wave, saved_wave, main, ends)),
    )
    return pl.pallas_call(
        finish,
        out_shape=(
            jax.ShapeDtypeStruct(fwd_wave.shape, F32),
            jax.ShapeDtypeStruct(adj_wave.shape, BF16),
            jax.ShapeDtypeStruct(potential.shape, F32),
        ),
        in_specs=[vmem, vmem, vmem],
        out_specs=(hbm, hbm, hbm),
        scratch_shapes=[pltpu.VMEM(fwd_wave.shape, F32), held(adj_wave), dma(4)],
        name="finish",
    )(near(wave_next), near(adj_next), near(gradient))


def solution(mesh):
    placed = (
        P("depth", "tile", None),
        P(),
        P("tile", None, None),
        P("tile", None, None, None),
        P("depth", "tile", None, None, None),
        P("depth", "tile", None, None, None),
        P("depth", "tile", None, None, None, None),
    )
    return jax.shard_map(
        functools.partial(on_device, mesh.shape["depth"], mesh.shape["tile"]),
        mesh=mesh,
        in_specs=placed,
        out_specs=(
            P("depth", "tile", None, None, None),
            P("depth", "tile", None, None, None),
            P("depth", "tile", None),
        ),
        check_vma=False,
    )
```

```python
import functools
import math

import jax
import jax.numpy as jnp
import numpy as np
from jax import lax
from jax.experimental import pallas as pl
from jax.experimental.pallas import tpu as pltpu
from jax.sharding import PartitionSpec as P

SIGMA = 0.8
DEFOCUS = 6.0
VTOP = 3.0
ROWS = 128
LANES = 128
STEP = 32
VLIM = 40
MESH = pl.DeviceIdType.MESH
F32 = jnp.float32
BF16 = jnp.bfloat16


def rounded(x):
    return x.real.astype(BF16).astype(np.float64) + 1j * x.imag.astype(BF16).astype(np.float64)


def left_blocks(x):
    n = x.shape[0]
    nc = n // ROWS
    out = np.zeros((nc, nc, 2 * ROWS, 2 * ROWS))
    for o in range(nc):
        for c in range(nc):
            b = x[o * ROWS : (o + 1) * ROWS, c * ROWS : (c + 1) * ROWS]
            out[o, c] = np.block([[b.real, -b.imag], [b.imag, b.real]])
    return out.transpose(0, 2, 1, 3).reshape(2 * n, 2 * n)


def right_block(x):
    return np.block([[x.real, x.imag], [-x.imag, x.real]])


def tables(n):
    idx = np.arange(n)
    angle = (idx[:, None] * idx[None, :] % n) * (2.0 * math.pi / n)
    scale = 1.0 / math.sqrt(n)
    cos_t = np.asarray((np.cos(angle) * scale).astype(BF16)).astype(np.float64)
    sin_t = np.asarray((np.sin(angle) * scale).astype(BF16)).astype(np.float64)
    freq = np.where(idx < n // 2, idx, idx - n).astype(np.float64)
    q = np.exp(-1j * math.pi * DEFOCUS * freq * freq / (n * n))
    f = cos_t - 1j * sin_t
    m = (np.conj(f) * q[None, :]) @ f
    m = (m + m.T) / 2
    best = (np.inf, 1.0)
    for size in np.linspace(0.7, 1.4, 64):
        z = (size * np.exp(1j * np.linspace(0.0, math.pi / 2, 128, endpoint=False)))[:, None]
        row = m[0][None, :]
        miss = np.sum(np.abs(rounded(row * z) - row * z) ** 2, axis=1) / size**2
        miss += np.sum(np.abs(rounded(row / z) - row / z) ** 2, axis=1) * size**2
        at = int(np.argmin(miss))
        if miss[at] < best[0]:
            best = (miss[at], z[at, 0])
    z = best[1]
    g = np.conj(f) * q[None, :]
    main = np.stack([left_blocks(z * m), right_block(m / z)]).astype(BF16)
    ends = [p for v in (f, g, g.T) for p in (v.real, v.imag)]
    return main, np.stack(ends).astype(BF16)


def sin_cos(v):
    mid = 0.5 * VTOP * SIGMA
    y = v * SIGMA - mid
    z = y * y
    s = y * (1.0 + z * (-1.0 / 6 + z * (1.0 / 120 + z * (-1.0 / 5040 + z * (1.0 / 362880)))))
    c = 1.0 + z * (-0.5 + z * (1.0 / 24 + z * (-1.0 / 720 + z * (1.0 / 40320))))
    sm, cm = math.sin(mid), math.cos(mid)
    return s * cm + c * sm, c * cm - s * sm


def dot(a, b):
    return jnp.dot(a, b, preferred_element_type=F32)


def kernel(
    sections, tiles,
    pos_h, pot_h, probe_h, inten_h, fwd_h, adj_h, saved_h, main_h, ends_h,
    o_fwd, o_adj, o_grad,
    in_f, in_b, out_f, out_b, out_r, main, l_f, r_f, l_g, r_g,
    cs, tf, ta, tv, bk, total, pad, y_buf,
    halo_out, halo_in, edge_out, edge_in, view_out, view_in, side_out, side_in,
    pos, pot, probe, inten, fwd, adj, saved, ends, load_sem,
    send_f, recv_f, send_b, recv_b, send_h, recv_h, send_e, recv_e, send_v, recv_v, send_r, send_s, recv_s, ready,
):
    n = probe.shape[1]
    nc = n // ROWS
    cols = n // LANES
    core, width = pot.shape[1], pot.shape[2]
    margin = (width - core) // 2
    ticks = inten.shape[1]
    s = lax.axis_index("depth")
    t = lax.axis_index("tile")
    first, last = s == 0, s == sections - 1
    low, high = t == 0, t == tiles - 1
    odd = lax.rem(s, 2) == 1
    relay = jnp.logical_and(odd, s > 1)
    aside = jnp.logical_and(jnp.logical_not(odd), jnp.logical_and(s > 0, s < sections - 1))
    ahead = jnp.logical_and(lax.rem(s, 2) == 0, s > 0)
    behind = jnp.logical_and(lax.rem(s, 2) == 1, s < sections - 1)

    loads = {}

    def load(name, src, dst):
        loads[name] = pltpu.make_async_copy(src, dst, load_sem.at[len(loads)])
        return loads[name]

    barrier = pltpu.get_barrier_semaphore()
    one = lambda c: jnp.where(c, 1, 0).astype(jnp.int32)

    def greet(cond, axis, to):
        @pl.when(cond)
        def _():
            pl.semaphore_signal(barrier, inc=1, device_id={axis: to}, device_id_type=MESH)

    greet(t > 0, "tile", t - 1)
    greet(t < tiles - 1, "tile", t + 1)
    greet(s < sections - 1, "depth", s + 1)
    greet(jnp.logical_and(odd, s < sections - 2), "depth", s + 2)
    load("pot", pot_h, pot).start()
    load("pos", pos_h, pos).start()
    load("main", main_h, main).start()
    load("adj", adj_h, adj).start()
    load("fwd", fwd_h, fwd).start()
    load("probe", probe_h, probe)
    load("ends", ends_h, ends)
    load("inten", inten_h, inten)

    @pl.when(first)
    def _():
        loads["probe"].start()

    @pl.when(last)
    def _():
        loads["ends"].start()
        loads["inten"].start()

    load("saved", saved_h, saved).start()
    loads["pot"].wait()
    halo_out[0] = pot[0, 0:margin, :].astype(BF16)
    halo_out[1] = pot[0, core - margin : core, :].astype(BF16)
    pl.semaphore_wait(barrier, one(s > 0) + one(relay) + one(t > 0) + one(t < tiles - 1))

    def hop(src, dst, ssem, rsem, axis, to):
        return pltpu.make_async_remote_copy(
            src_ref=src, dst_ref=dst, send_sem=ssem, recv_sem=rsem,
            device_id={axis: to}, device_id_type=MESH,
        )

    def tile_pair(src, dst, ssem, rsem):
        down = hop(src.at[0], dst.at[1], ssem.at[0], rsem.at[1], "tile", t - 1)
        up = hop(src.at[1], dst.at[0], ssem.at[1], rsem.at[0], "tile", t + 1)
        return down, up

    def tile_start(src, dst, ssem, rsem):
        down, up = tile_pair(src, dst, ssem, rsem)
        pl.when(t > 0)(down.start)
        pl.when(t < tiles - 1)(up.start)

    def tile_wait(src, dst, ssem, rsem):
        down, up = tile_pair(src, dst, ssem, rsem)

        @pl.when(t > 0)
        def _():
            down.wait_send()
            up.wait_recv()

        @pl.when(t < tiles - 1)
        def _():
            up.wait_send()
            down.wait_recv()

    tile_start(halo_out, halo_in, send_h, recv_h)

    @pl.when(s > 0)
    def _():
        pl.semaphore_signal(ready, inc=1, device_id={"depth": s - 1}, device_id_type=MESH)

    def stacked(x):
        return x.reshape(2 * ROWS, n)

    def m_left(o, c):
        return main[0, o * 2 * ROWS : (o + 1) * 2 * ROWS, c * 2 * ROWS : (c + 1) * 2 * ROWS]

    def product(get_left, get_x, r_ref, sink):
        acc = [None] * nc
        for c in range(nc):
            x = get_x(c)
            for o in range(nc):
                term = dot(get_left(o, c), x)
                acc[o] = term if acc[o] is None else acc[o] + term
        for o in range(nc):
            a = acc[o].astype(BF16)
            out = dot(jnp.concatenate([a[0:ROWS, :], a[ROWS : 2 * ROWS, :]], axis=1), r_ref[...])
            sink(o, out[:, 0:n], out[:, n : 2 * n])

    def copy_f(k, c):
        return hop(out_f.at[k, c], in_f.at[k + 1, c], send_f.at[k, c], recv_f.at[k, c], "depth", s + 1)

    def copy_b(k, c):
        return hop(out_b.at[k, c], in_b.at[k + 1, c], send_b.at[k, c], recv_b.at[k, c], "depth", s - 1)

    def copy_r(k, c):
        return hop(out_r.at[k, c], in_b.at[k + 2, c], send_r.at[k, c], recv_b.at[k + 1, c], "depth", s - 2)

    def last_r(c):
        k, rows = ticks - 2, slice(c * ROWS, (c + 1) * ROWS)
        return hop(out_r.at[k, c], o_adj.at[0, 0, :, rows, :], send_r.at[k, c], recv_b.at[k + 1, c], "depth", s - 2)

    def copy_s(k, c):
        return hop(side_out.at[k, c], side_in.at[k, c], send_s.at[k, c], recv_s.at[k, c], "depth", s + 1)

    def last_b(c):
        k, rows = ticks - 1, slice(c * ROWS, (c + 1) * ROWS)
        return hop(out_b.at[k, c], o_adj.at[0, 0, :, rows, :], send_b.at[k, c], recv_b.at[k, c], "depth", s - 1)

    loads["adj"].wait()
    for c in range(nc):
        rows = slice(c * ROWS, (c + 1) * ROWS)
        in_b[0, c, 0] = adj[0, 0, 0, rows, :]
        in_b[0, c, 1] = -adj[0, 0, 1, rows, :]
    loads["main"].wait()

    def keep(o, lur, lui):
        rows = slice(o * ROWS, (o + 1) * ROWS)
        bk[0, rows, :] = lur
        bk[1, rows, :] = lui
        out_b[0, o, 0] = lur.astype(BF16)
        out_b[0, o, 1] = lui.astype(BF16)
        pl.when(ahead)(lambda: copy_b(0, o).start())

    product(m_left, lambda c: stacked(in_b[0, c]), main.at[1], keep)

    def place(part, at, x):
        for i in range(cols + 1):
            cs[i, pl.ds(3 * at + part, STEP, stride=3), :] = x[:, i * LANES : (i + 1) * LANES]

    def phase_table(at, v):
        sv, cv = sin_cos(v)
        place(0, at, cv)
        place(1, at, sv)

    for at in range(0, core, STEP):
        place(2, margin + at, pot[0, at : at + STEP, :])
        phase_table(margin + at, pot[0, at : at + STEP, :])
    total[...] = jnp.zeros_like(total)
    spare = width - n
    for i in range(cols + 1):
        pad[i, 0 : 2 * spare, :] = jnp.zeros((2 * spare, LANES), F32)
        pad[i, 2 * (spare + n) :, :] = jnp.zeros((2 * spare, LANES), F32)
    loads["fwd"].wait()
    for c in range(nc):
        rows = slice(c * ROWS, (c + 1) * ROWS)
        for part in range(2):
            in_f[0, c, part] = fwd[0, 0, part, rows, :].astype(BF16)

    @pl.when(first)
    def _():
        loads["probe"].wait()
        for k in range(ticks):
            for c in range(nc):
                for part in range(2):
                    in_f[k + 1, c, part] = probe[part, c * ROWS : (c + 1) * ROWS, :]

    @pl.when(last)
    def _():
        loads["ends"].wait()
        loads["inten"].wait()

        def fill_left(ref, xr, xi):
            for o in range(nc):
                for c in range(nc):
                    br = xr[o * ROWS : (o + 1) * ROWS, c * ROWS : (c + 1) * ROWS]
                    bi = xi[o * ROWS : (o + 1) * ROWS, c * ROWS : (c + 1) * ROWS]
                    ref[o, c, 0:ROWS, 0:ROWS] = br
                    ref[o, c, 0:ROWS, ROWS : 2 * ROWS] = -bi
                    ref[o, c, ROWS : 2 * ROWS, 0:ROWS] = bi
                    ref[o, c, ROWS : 2 * ROWS, ROWS : 2 * ROWS] = br

        def fill_right(ref, xr, xi):
            ref[0:n, 0:n] = xr
            ref[0:n, n : 2 * n] = xi
            ref[n : 2 * n, 0:n] = -xi
            ref[n : 2 * n, n : 2 * n] = xr

        fill_left(l_f, ends[0], ends[1])
        fill_right(r_f, ends[0], ends[1])
        fill_left(l_g, ends[2], ends[3])
        fill_right(r_g, ends[4], ends[5])

    @pl.when(low)
    def _():
        halo_in[0] = jnp.zeros((margin, width), BF16)
        edge_in[0] = jnp.zeros((margin, width), BF16)

    @pl.when(high)
    def _():
        halo_in[1] = jnp.zeros((margin, width), BF16)
        edge_in[1] = jnp.zeros((margin, width), BF16)

    loads["pos"].wait()
    tile_wait(halo_out, halo_in, send_h, recv_h)
    strips = [(side * (margin + core) + at, side, slice(at, at + STEP)) for side in range(2) for at in range(0, margin, STEP)]
    for at, side, rows in strips:
        place(2, at, halo_in[side, rows, :].astype(F32))

    lane = lax.broadcasted_iota(jnp.int32, (STEP, LANES), 1)

    def window(index, parts, store, steps=range(0, n, STEP)):
        r, c = pos[0, 0, index], pos[0, 1, index]
        turn = lax.rem(LANES - c, LANES)
        own = lane < LANES - c
        for part in parts:
            for at in steps:
                rows = pl.ds(3 * (r + at) + part, STEP, stride=3)
                x = [pltpu.roll(cs[i, rows, :], turn, 1) for i in range(cols + 1)]
                for i in range(cols):
                    store(part, at, slice(i * LANES, (i + 1) * LANES), jnp.where(own, x[i], x[i + 1]))

    def window_b(k):
        def store(part, at, tile, x):
            ta[lax.rem(k, 2), part, at : at + STEP, tile] = x
        window(k + s, range(2), store)

    def window_f(k):
        def store(part, at, tile, x):
            tf[lax.rem(k, 2), part, at : at + STEP, tile] = x
        window(k - s + 2 * sections - 1, range(2), store)

    def copy_v(c):
        return hop(view_out.at[c], view_in.at[c], send_v.at[c], recv_v.at[c], "depth", s - 1)

    def send_views(index, out, copy):
        def store(part, at, tile, x):
            out[at // ROWS, at % ROWS : at % ROWS + STEP, tile] = x.astype(BF16)
        for c in range(nc):
            window(index, (2,), store, range(c * ROWS, (c + 1) * ROWS, STEP))
            copy(c).start()

    def send_aside(k):
        send_views(k + s + 1, side_out.at[k], functools.partial(copy_s, k))

    def side_phase(k):
        for c in range(nc):
            copy_s(k, c).wait_recv()
            for at in range(0, ROWS, STEP):
                sv, cv = sin_cos(side_in[k, c, at : at + STEP, :].astype(F32))
                rows = slice(c * ROWS + at, c * ROWS + at + STEP)
                tv[lax.rem(k, 2), 0, rows, :] = cv
                tv[lax.rem(k, 2), 1, rows, :] = sv

    def windows(k):
        window_b(k)
        window_f(k)

    def scatter(k):
        r, c = pos[0, 0, k + s], pos[0, 1, k + s]
        own = lane >= c
        turn = lax.rem(c, LANES)
        def lay(lo, hi):
            for at in range(lo, hi, STEP):
                rows = slice(at, at + STEP)
                sr = saved[0, 0, k, 0, rows, :].astype(F32)
                si = saved[0, 0, k, 1, rows, :].astype(F32)
                d = (bk[1, rows, :] * sr + bk[0, rows, :] * si) * -SIGMA
                d = [pltpu.roll(d[:, i * LANES : (i + 1) * LANES], turn, 1) for i in range(cols)]
                zero = jnp.zeros((STEP, LANES), F32)
                d = [zero] + d + [zero]
                for i in range(cols + 1):
                    pad[i, pl.ds(2 * (spare + at), STEP, stride=2), :] = jnp.where(own, d[i + 1], d[i])

        def add(lo, hi):
            for at in range(lo, hi, STEP):
                for i in range(cols + 1):
                    total[at : at + STEP, i * LANES : (i + 1) * LANES] += pad[
                        i, pl.ds(2 * (spare - r + at), STEP, stride=2), :
                    ]

        lay(0, margin)
        lay(n - margin, n)
        add(0, margin)
        add(margin + core, width)
        if not isinstance(k, int):
            @pl.when(k == ticks - 1)
            def _():
                edge_out[0] = total[0:margin, :].astype(BF16)
                edge_out[1] = total[margin + core :, :].astype(BF16)
                tile_start(edge_out, edge_in, send_e, recv_e)
        lay(margin, n - margin)
        add(margin, margin + core)

    def send_back(k, c, lur, lui):
        rows = slice(c * ROWS, (c + 1) * ROWS)
        slot = lax.rem(k, 2)
        tr, ti = ta[slot, 0, rows, :], ta[slot, 1, rows, :]
        br = tr * lur - ti * lui
        bi = tr * lui + ti * lur
        bk[0, rows, :] = br
        bk[1, rows, :] = bi

        if isinstance(k, int):
            @pl.when(odd)
            def _():
                out_b[k, c, 0] = br.astype(BF16)
                out_b[k, c, 1] = bi.astype(BF16)
                copy_b(k, c).start()
            return

        @pl.when(odd)
        def _():
            out_b[k, c, 0] = br.astype(BF16)
            out_b[k, c, 1] = (bi * jnp.where(k == ticks - 1, -1.0, 1.0)).astype(BF16)
            pl.when(k < ticks - 1)(lambda: copy_b(k, c).start())
            pl.when(k == ticks - 1)(lambda: last_b(c).start())

    def backward(k):
        def arrived(c):
            @pl.when(jnp.logical_not(last))
            def _():
                copy_b(k - 1, c).wait_recv()

            @pl.when(jnp.logical_and(k == 1, behind))
            def _():
                copy_v(c).wait_recv()
                lur, lui = in_b[1, c, 0].astype(F32), in_b[1, c, 1].astype(F32)
                ti, tr = sin_cos(view_in[c].astype(F32))
                in_b[1, c, 0] = (tr * lur - ti * lui).astype(BF16)
                in_b[1, c, 1] = (tr * lui + ti * lur).astype(BF16)
            return stacked(in_b[k, c])

        product(m_left, arrived, main.at[1], functools.partial(send_back, k))

    def pass_on(k):
        def sink(c, lur, lui):
            rows = slice(c * ROWS, (c + 1) * ROWS)
            slot = lax.rem(k, 2)
            tr, ti = tv[slot, 0, rows, :], tv[slot, 1, rows, :]
            out_r[k, c, 0] = (tr * lur - ti * lui).astype(BF16)
            bi = tr * lui + ti * lur
            if isinstance(k, int):
                out_r[k, c, 1] = bi.astype(BF16)
                copy_r(k, c).start()
            else:
                out_r[k, c, 1] = (bi * jnp.where(k == ticks - 2, -1.0, 1.0)).astype(BF16)
                pl.when(k < ticks - 2)(lambda: copy_r(k, c).start())
                pl.when(k == ticks - 2)(lambda: last_r(c).start())

        product(m_left, lambda c: stacked(out_b[k, c]), main.at[1], sink)

    def entering(k, c, waits):
        if waits:
            @pl.when(jnp.logical_not(first))
            def _():
                copy_f(k - 1, c).wait_recv()
        rows = slice(c * ROWS, (c + 1) * ROWS)
        slot = lax.rem(k, 2)
        wr, wi = in_f[k, c, 0].astype(F32), in_f[k, c, 1].astype(F32)
        tr, ti = tf[slot, 0, rows, :], tf[slot, 1, rows, :]
        return jnp.concatenate([tr * wr - ti * wi, tr * wi + ti * wr], axis=0).astype(BF16)

    def forward(k, waits=True):
        def sink(c, outr, outi):
            out_f[k, c, 0] = outr.astype(BF16)
            out_f[k, c, 1] = outi.astype(BF16)
            copy_f(k, c).start()

        product(m_left, lambda c: entering(k, c, waits), main.at[1], sink)

    def forward_last(k, waits=True):
        def detect(c, vr, vi):
            rows = slice(c * ROWS, (c + 1) * ROWS)
            excess = vr * vr + vi * vi - inten[0, k, rows, :].astype(F32)
            y_buf[c, 0:ROWS, :] = (excess * vr).astype(BF16)
            y_buf[c, ROWS : 2 * ROWS, :] = (excess * vi).astype(BF16)

        def seed(c, outr, outi):
            in_b[k + 1, c, 0] = outr.astype(BF16)
            in_b[k + 1, c, 1] = -outi.astype(BF16)

        product(lambda o, c: l_f[o, c], lambda c: entering(k, c, waits), r_f, detect)
        product(lambda o, c: l_g[o, c], lambda c: y_buf[c], r_g, seed)

    @pl.when(ahead)
    def _():
        send_views(s, view_out, copy_v)

    @pl.when(jnp.logical_not(last))
    def _():
        pl.semaphore_wait(ready, 1)

    pl.when(aside)(lambda: send_aside(0))
    for at, side, rows in strips:
        phase_table(at, halo_in[side, rows, :].astype(F32))
    window_b(0)
    for c in range(nc):
        rows = slice(c * ROWS, (c + 1) * ROWS)
        send_back(0, c, bk[0, rows, :], bk[1, rows, :])
    window_f(0)

    @pl.when(jnp.logical_not(last))
    def _():
        forward(0, False)

    @pl.when(last)
    def _():
        forward_last(0, False)

    @pl.when(relay)
    def _():
        side_phase(0)
        pass_on(0)

    @pl.when(aside)
    def _():
        for k in range(1, ticks - 1):
            send_aside(k)

    windows(1)
    pl.when(relay)(lambda: side_phase(1))
    loads["saved"].wait()
    scatter(0)

    early = jnp.logical_or(first, jnp.logical_and(lax.rem(s, 2) == 1, jnp.logical_not(last)))

    @pl.when(early)
    def _():
        def tick(k, carry):
            forward(k)

            @pl.when(k < ticks - 1)
            def _():
                windows(k + 1)
            pl.when(jnp.logical_and(relay, k < ticks - 2))(lambda: side_phase(k + 1))
            backward(k)
            pl.when(jnp.logical_and(relay, k < ticks - 1))(lambda: pass_on(k))
            scatter(k)
            return carry
        lax.fori_loop(1, ticks, tick, 0)

    @pl.when(jnp.logical_not(early))
    def _():
        def tick(k, carry):
            backward(k)
            pl.when(jnp.logical_and(relay, k < ticks - 1))(lambda: pass_on(k))
            scatter(k)

            @pl.when(k < ticks - 1)
            def _():
                windows(k + 1)
            pl.when(jnp.logical_and(relay, k < ticks - 2))(lambda: side_phase(k + 1))

            @pl.when(jnp.logical_not(last))
            def _():
                forward(k)

            @pl.when(last)
            def _():
                forward_last(k)
            return carry
        lax.fori_loop(1, ticks, tick, 0)

    o_grad[0, margin : core - margin, :] = total[2 * margin : core, :]
    for c in range(nc):
        @pl.when(jnp.logical_not(first))
        def _():
            copy_f(ticks - 1, c).wait_recv()
        o_fwd[0, 0, :, c * ROWS : (c + 1) * ROWS, :] = in_f[ticks, c].astype(F32)
    tile_wait(edge_out, edge_in, send_e, recv_e)
    o_grad[0, 0:margin, :] = total[margin : 2 * margin, :] + edge_in[0].astype(F32)
    o_grad[0, core - margin : core, :] = total[core : core + margin, :] + edge_in[1].astype(F32)

    @pl.when(last)
    def _():
        for c in range(nc):
            rows = slice(c * ROWS, (c + 1) * ROWS)
            o_adj[0, 0, 0, rows, :] = in_b[ticks, c, 0]
            o_adj[0, 0, 1, rows, :] = -in_b[ticks, c, 1]

    @pl.when(jnp.logical_not(last))
    def _():
        for c in range(nc):
            last_b(c).wait_recv()

    for c in range(nc):
        @pl.when(ahead)
        def _():
            copy_v(c).wait_send()
            copy_b(0, c).wait_send()

        for k in range(ticks):
            pl.when(jnp.logical_not(last))(lambda: copy_f(k, c).wait_send())
            pl.when(odd)(lambda: copy_b(k, c).wait_send())
        for k in range(ticks - 1):
            pl.when(relay)(lambda: copy_r(k, c).wait_send())
            pl.when(aside)(lambda: copy_s(k, c).wait_send())


def finish(wave, adj, grad, o_wave, o_adj, o_grad, sem):
    moves = [
        pltpu.make_async_copy(src, dst, sem.at[i])
        for i, (src, dst) in enumerate(((wave, o_wave), (grad, o_grad), (adj, o_adj)))
    ]
    for move in moves:
        move.start()
    for move in moves:
        move.wait()


def on_device(sections, tiles, potential, probe, positions, intensity, fwd_wave, adj_wave, saved_wave):
    n = probe.shape[1]
    nc = n // ROWS
    ticks = intensity.shape[1]
    core, width = potential.shape[1], potential.shape[2]
    margin = (width - core) // 2
    main, ends = (jnp.asarray(x) for x in tables(n))
    held = lambda x: pltpu.VMEM(x.shape, x.dtype)
    vmem = pl.BlockSpec(memory_space=pltpu.VMEM)
    spots = jnp.swapaxes(positions, 1, 2)
    hbm = pl.BlockSpec(memory_space=pltpu.HBM)
    dma = lambda *shape: pltpu.SemaphoreType.DMA(shape)
    far = lambda x: pltpu.with_memory_space_constraint(x, pltpu.HBM)
    near = lambda x: pltpu.with_memory_space_constraint(x, pltpu.VMEM)
    wave = lambda count: pltpu.VMEM((count, nc, 2, ROWS, n), BF16)
    lt = pltpu.VMEM((nc, nc, 2 * ROWS, 2 * ROWS), BF16)
    rt = pltpu.VMEM((2 * n, 2 * n), BF16)
    square = pltpu.VMEM((width, width), F32)
    pair = pltpu.VMEM((2, 2, n, n), F32)
    view = lambda *count: pltpu.VMEM((*count, ROWS, n), BF16)
    strip = pltpu.VMEM((2, margin, width), BF16)
    wave_next, adj_next, gradient = pl.pallas_call(
        functools.partial(kernel, sections, tiles),
        out_shape=(
            pltpu.VMEM(fwd_wave.shape, F32),
            pltpu.VMEM(adj_wave.shape, BF16),
            pltpu.VMEM(potential.shape, F32),
        ),
        in_specs=[hbm] * 9,
        out_specs=(vmem, vmem, vmem),
        scratch_shapes=[
            wave(ticks + 1), wave(ticks + 1), wave(ticks), wave(ticks), wave(ticks - 1),
            held(main), lt, rt, lt, rt,
            pltpu.VMEM((width // LANES, 3 * width, LANES), F32), pair, pair, pair, pltpu.VMEM((2, n, n), F32),
            square, pltpu.VMEM((width // LANES, 4 * width - 2 * n, LANES), F32),
            pltpu.VMEM((nc, 2 * ROWS, n), BF16),
            strip, strip, strip, strip, view(nc), view(nc),
            view(ticks - 1, nc), view(ticks - 1, nc),
            pltpu.SMEM(spots.shape, spots.dtype), held(potential), held(probe), held(intensity), held(fwd_wave), held(adj_wave),
            held(saved_wave), held(ends), dma(9),
            dma(ticks, nc), dma(ticks, nc), dma(ticks, nc), dma(ticks, nc),
            dma(2), dma(2), dma(2), dma(2), dma(nc), dma(nc),
            dma(ticks - 1, nc), dma(ticks - 1, nc), dma(ticks - 1, nc), pltpu.SemaphoreType.REGULAR,
        ],
        compiler_params=pltpu.CompilerParams(
            collective_id=0, has_side_effects=True, vmem_limit_bytes=VLIM * 1024 * 1024
        ),
        name="window",
    )(
        *(far(x) for x in (spots, potential, probe, intensity, fwd_wave, adj_wave, saved_wave, main, ends)),
    )
    return pl.pallas_call(
        finish,
        out_shape=(
            jax.ShapeDtypeStruct(fwd_wave.shape, F32),
            jax.ShapeDtypeStruct(adj_wave.shape, BF16),
            jax.ShapeDtypeStruct(potential.shape, F32),
        ),
        in_specs=[vmem, vmem, vmem],
        out_specs=(hbm, hbm, hbm),
        scratch_shapes=[dma(3)],
        name="finish",
    )(near(wave_next), near(adj_next), near(gradient))


def solution(mesh):
    placed = (
        P("depth", "tile", None),
        P(),
        P("tile", None, None),
        P("tile", None, None, None),
        P("depth", "tile", None, None, None),
        P("depth", "tile", None, None, None),
        P("depth", "tile", None, None, None, None),
    )
    return jax.shard_map(
        functools.partial(on_device, mesh.shape["depth"], mesh.shape["tile"]),
        mesh=mesh,
        in_specs=placed,
        out_specs=(
            P("depth", "tile", None, None, None),
            P("depth", "tile", None, None, None),
            P("depth", "tile", None),
        ),
        check_vma=False,
    )
```

```python
import functools
import math

import jax
import jax.numpy as jnp
import numpy as np
from jax import lax
from jax.experimental import pallas as pl
from jax.experimental.pallas import tpu as pltpu
from jax.sharding import PartitionSpec as P

SIGMA = 0.8
DEFOCUS = 6.0
VTOP = 3.0
ROWS = 128
LANES = 128
STEP = 32
VLIM = 40
MESH = pl.DeviceIdType.MESH
F32 = jnp.float32
BF16 = jnp.bfloat16


def rounded(x):
    return x.real.astype(BF16).astype(np.float64) + 1j * x.imag.astype(BF16).astype(np.float64)


def left_blocks(x):
    n = x.shape[0]
    nc = n // ROWS
    out = np.zeros((nc, nc, 2 * ROWS, 2 * ROWS))
    for o in range(nc):
        for c in range(nc):
            b = x[o * ROWS : (o + 1) * ROWS, c * ROWS : (c + 1) * ROWS]
            out[o, c] = np.block([[b.real, -b.imag], [b.imag, b.real]])
    return out.transpose(0, 2, 1, 3).reshape(2 * n, 2 * n)


def right_block(x):
    return np.block([[x.real, x.imag], [-x.imag, x.real]])


def tables(n):
    idx = np.arange(n)
    angle = (idx[:, None] * idx[None, :] % n) * (2.0 * math.pi / n)
    scale = 1.0 / math.sqrt(n)
    cos_t = np.asarray((np.cos(angle) * scale).astype(BF16)).astype(np.float64)
    sin_t = np.asarray((np.sin(angle) * scale).astype(BF16)).astype(np.float64)
    freq = np.where(idx < n // 2, idx, idx - n).astype(np.float64)
    q = np.exp(-1j * math.pi * DEFOCUS * freq * freq / (n * n))
    f = cos_t - 1j * sin_t
    m = (np.conj(f) * q[None, :]) @ f
    m = (m + m.T) / 2
    best = (np.inf, 1.0)
    for size in np.linspace(0.7, 1.4, 64):
        z = (size * np.exp(1j * np.linspace(0.0, math.pi / 2, 128, endpoint=False)))[:, None]
        row = m[0][None, :]
        miss = np.sum(np.abs(rounded(row * z) - row * z) ** 2, axis=1) / size**2
        miss += np.sum(np.abs(rounded(row / z) - row / z) ** 2, axis=1) * size**2
        at = int(np.argmin(miss))
        if miss[at] < best[0]:
            best = (miss[at], z[at, 0])
    z = best[1]
    g = np.conj(f) * q[None, :]
    main = np.stack([left_blocks(z * m), right_block(m / z)]).astype(BF16)
    ends = [p for v in (f, g, g.T) for p in (v.real, v.imag)]
    return main, np.stack(ends).astype(BF16)


def sin_cos(v):
    mid = 0.5 * VTOP * SIGMA
    y = v * SIGMA - mid
    z = y * y
    s = y * (1.0 + z * (-1.0 / 6 + z * (1.0 / 120 + z * (-1.0 / 5040 + z * (1.0 / 362880)))))
    c = 1.0 + z * (-0.5 + z * (1.0 / 24 + z * (-1.0 / 720 + z * (1.0 / 40320))))
    sm, cm = math.sin(mid), math.cos(mid)
    return s * cm + c * sm, c * cm - s * sm


def dot(a, b):
    return jnp.dot(a, b, preferred_element_type=F32)


def kernel(
    sections, tiles,
    pos_h, pot_h, probe_h, inten_h, fwd_h, adj_h, saved_h, main_h, ends_h,
    o_fwd, o_adj, o_grad,
    in_f, in_b, out_f, out_b, out_r, main, l_f, r_f, l_g, r_g,
    cs, tf, ta, tv, bk, total, pad, y_buf,
    halo_out, halo_in, edge_out, edge_in, view_out, view_in, side_out, side_in,
    pos, pot, probe, inten, fwd, adj, saved, ends, load_sem,
    send_f, recv_f, send_b, recv_b, send_h, recv_h, send_e, recv_e, send_v, recv_v, send_r, send_s, recv_s, ready,
):
    n = probe.shape[1]
    nc = n // ROWS
    cols = n // LANES
    core, width = pot.shape[1], pot.shape[2]
    margin = (width - core) // 2
    ticks = inten.shape[1]
    s = lax.axis_index("depth")
    t = lax.axis_index("tile")
    first, last = s == 0, s == sections - 1
    low, high = t == 0, t == tiles - 1
    odd = lax.rem(s, 2) == 1
    relay = jnp.logical_and(odd, s > 1)
    aside = jnp.logical_and(jnp.logical_not(odd), jnp.logical_and(s > 0, s < sections - 1))
    ahead = jnp.logical_and(lax.rem(s, 2) == 0, s > 0)
    behind = jnp.logical_and(lax.rem(s, 2) == 1, s < sections - 1)

    loads = {}

    def load(name, src, dst):
        loads[name] = pltpu.make_async_copy(src, dst, load_sem.at[len(loads)])
        return loads[name]

    barrier = pltpu.get_barrier_semaphore()
    one = lambda c: jnp.where(c, 1, 0).astype(jnp.int32)

    def greet(cond, axis, to):
        @pl.when(cond)
        def _():
            pl.semaphore_signal(barrier, inc=1, device_id={axis: to}, device_id_type=MESH)

    greet(t > 0, "tile", t - 1)
    greet(t < tiles - 1, "tile", t + 1)
    greet(s < sections - 1, "depth", s + 1)
    greet(jnp.logical_and(odd, s < sections - 2), "depth", s + 2)
    load("pot", pot_h, pot).start()
    load("pos", pos_h, pos).start()
    load("main", main_h, main).start()
    load("adj", adj_h, adj).start()
    load("fwd", fwd_h, fwd).start()
    load("probe", probe_h, probe)
    load("ends", ends_h, ends)
    load("inten", inten_h, inten)

    @pl.when(first)
    def _():
        loads["probe"].start()

    @pl.when(last)
    def _():
        loads["ends"].start()
        loads["inten"].start()

    load("saved", saved_h, saved).start()
    loads["pot"].wait()
    halo_out[0] = pot[0, 0:margin, :].astype(BF16)
    halo_out[1] = pot[0, core - margin : core, :].astype(BF16)
    pl.semaphore_wait(barrier, one(s > 0) + one(relay) + one(t > 0) + one(t < tiles - 1))

    def hop(src, dst, ssem, rsem, axis, to):
        return pltpu.make_async_remote_copy(
            src_ref=src, dst_ref=dst, send_sem=ssem, recv_sem=rsem,
            device_id={axis: to}, device_id_type=MESH,
        )

    def tile_pair(src, dst, ssem, rsem):
        down = hop(src.at[0], dst.at[1], ssem.at[0], rsem.at[1], "tile", t - 1)
        up = hop(src.at[1], dst.at[0], ssem.at[1], rsem.at[0], "tile", t + 1)
        return down, up

    def tile_down(*refs):
        pl.when(t > 0)(tile_pair(*refs)[0].start)

    def tile_up(*refs):
        pl.when(t < tiles - 1)(tile_pair(*refs)[1].start)

    def tile_start(src, dst, ssem, rsem):
        tile_down(src, dst, ssem, rsem)
        tile_up(src, dst, ssem, rsem)

    def tile_wait(src, dst, ssem, rsem):
        down, up = tile_pair(src, dst, ssem, rsem)

        @pl.when(t > 0)
        def _():
            down.wait_send()
            up.wait_recv()

        @pl.when(t < tiles - 1)
        def _():
            up.wait_send()
            down.wait_recv()

    tile_start(halo_out, halo_in, send_h, recv_h)

    @pl.when(s > 0)
    def _():
        pl.semaphore_signal(ready, inc=1, device_id={"depth": s - 1}, device_id_type=MESH)

    def stacked(x):
        return x.reshape(2 * ROWS, n)

    def m_left(o, c):
        return main[0, o * 2 * ROWS : (o + 1) * 2 * ROWS, c * 2 * ROWS : (c + 1) * 2 * ROWS]

    def product(get_left, get_x, r_ref, sink):
        acc = [None] * nc
        for c in range(nc):
            x = get_x(c)
            for o in range(nc):
                term = dot(get_left(o, c), x)
                acc[o] = term if acc[o] is None else acc[o] + term
        for o in range(nc):
            a = acc[o].astype(BF16)
            out = dot(jnp.concatenate([a[0:ROWS, :], a[ROWS : 2 * ROWS, :]], axis=1), r_ref[...])
            sink(o, out[:, 0:n], out[:, n : 2 * n])

    def copy_f(k, c):
        return hop(out_f.at[k, c], in_f.at[k + 1, c], send_f.at[k, c], recv_f.at[k, c], "depth", s + 1)

    def copy_b(k, c):
        return hop(out_b.at[k, c], in_b.at[k + 1, c], send_b.at[k, c], recv_b.at[k, c], "depth", s - 1)

    def copy_r(k, c):
        return hop(out_r.at[k, c], in_b.at[k + 2, c], send_r.at[k, c], recv_b.at[k + 1, c], "depth", s - 2)

    def last_r(c):
        k, rows = ticks - 2, slice(c * ROWS, (c + 1) * ROWS)
        return hop(out_r.at[k, c], o_adj.at[0, 0, :, rows, :], send_r.at[k, c], recv_b.at[k + 1, c], "depth", s - 2)

    def copy_s(k, c):
        return hop(side_out.at[k, c], side_in.at[k, c], send_s.at[k, c], recv_s.at[k, c], "depth", s + 1)

    def last_b(c):
        k, rows = ticks - 1, slice(c * ROWS, (c + 1) * ROWS)
        return hop(out_b.at[k, c], o_adj.at[0, 0, :, rows, :], send_b.at[k, c], recv_b.at[k, c], "depth", s - 1)

    loads["adj"].wait()
    for c in range(nc):
        rows = slice(c * ROWS, (c + 1) * ROWS)
        in_b[0, c, 0] = adj[0, 0, 0, rows, :]
        in_b[0, c, 1] = -adj[0, 0, 1, rows, :]
    loads["main"].wait()

    def keep(o, lur, lui):
        rows = slice(o * ROWS, (o + 1) * ROWS)
        bk[0, rows, :] = lur
        bk[1, rows, :] = lui
        out_b[0, o, 0] = lur.astype(BF16)
        out_b[0, o, 1] = lui.astype(BF16)
        pl.when(ahead)(lambda: copy_b(0, o).start())

    product(m_left, lambda c: stacked(in_b[0, c]), main.at[1], keep)

    def place(part, at, x):
        for i in range(cols + 1):
            cs[i, pl.ds(3 * at + part, STEP, stride=3), :] = x[:, i * LANES : (i + 1) * LANES]

    def phase_table(at, v):
        sv, cv = sin_cos(v)
        place(0, at, cv)
        place(1, at, sv)

    for at in range(0, core, STEP):
        place(2, margin + at, pot[0, at : at + STEP, :])
        phase_table(margin + at, pot[0, at : at + STEP, :])
    total[...] = jnp.zeros_like(total)
    spare = width - n
    for i in range(cols + 1):
        pad[i, 0 : 2 * spare, :] = jnp.zeros((2 * spare, LANES), F32)
        pad[i, 2 * (spare + n) :, :] = jnp.zeros((2 * spare, LANES), F32)
    loads["fwd"].wait()
    for c in range(nc):
        rows = slice(c * ROWS, (c + 1) * ROWS)
        for part in range(2):
            in_f[0, c, part] = fwd[0, 0, part, rows, :].astype(BF16)

    @pl.when(first)
    def _():
        loads["probe"].wait()
        for k in range(ticks):
            for c in range(nc):
                for part in range(2):
                    in_f[k + 1, c, part] = probe[part, c * ROWS : (c + 1) * ROWS, :]

    @pl.when(last)
    def _():
        loads["ends"].wait()
        loads["inten"].wait()

        def fill_left(ref, xr, xi):
            for o in range(nc):
                for c in range(nc):
                    br = xr[o * ROWS : (o + 1) * ROWS, c * ROWS : (c + 1) * ROWS]
                    bi = xi[o * ROWS : (o + 1) * ROWS, c * ROWS : (c + 1) * ROWS]
                    ref[o, c, 0:ROWS, 0:ROWS] = br
                    ref[o, c, 0:ROWS, ROWS : 2 * ROWS] = -bi
                    ref[o, c, ROWS : 2 * ROWS, 0:ROWS] = bi
                    ref[o, c, ROWS : 2 * ROWS, ROWS : 2 * ROWS] = br

        def fill_right(ref, xr, xi):
            ref[0:n, 0:n] = xr
            ref[0:n, n : 2 * n] = xi
            ref[n : 2 * n, 0:n] = -xi
            ref[n : 2 * n, n : 2 * n] = xr

        fill_left(l_f, ends[0], ends[1])
        fill_right(r_f, ends[0], ends[1])
        fill_left(l_g, ends[2], ends[3])
        fill_right(r_g, ends[4], ends[5])

    @pl.when(low)
    def _():
        halo_in[0] = jnp.zeros((margin, width), BF16)
        edge_in[0] = jnp.zeros((margin, width), BF16)

    @pl.when(high)
    def _():
        halo_in[1] = jnp.zeros((margin, width), BF16)
        edge_in[1] = jnp.zeros((margin, width), BF16)

    loads["pos"].wait()
    tile_wait(halo_out, halo_in, send_h, recv_h)
    strips = [(side * (margin + core) + at, side, slice(at, at + STEP)) for side in range(2) for at in range(0, margin, STEP)]
    for at, side, rows in strips:
        place(2, at, halo_in[side, rows, :].astype(F32))

    lane = lax.broadcasted_iota(jnp.int32, (STEP, LANES), 1)

    def window(index, parts, store, steps=range(0, n, STEP)):
        r, c = pos[0, 0, index], pos[0, 1, index]
        turn = lax.rem(LANES - c, LANES)
        own = lane < LANES - c
        for part in parts:
            for at in steps:
                rows = pl.ds(3 * (r + at) + part, STEP, stride=3)
                x = [pltpu.roll(cs[i, rows, :], turn, 1) for i in range(cols + 1)]
                for i in range(cols):
                    store(part, at, slice(i * LANES, (i + 1) * LANES), jnp.where(own, x[i], x[i + 1]))

    def window_b(k):
        def store(part, at, tile, x):
            ta[lax.rem(k, 2), part, at : at + STEP, tile] = x
        window(k + s, range(2), store)

    def window_f(k):
        def store(part, at, tile, x):
            tf[lax.rem(k, 2), part, at : at + STEP, tile] = x
        window(k - s + 2 * sections - 1, range(2), store)

    def copy_v(c):
        return hop(view_out.at[c], view_in.at[c], send_v.at[c], recv_v.at[c], "depth", s - 1)

    def send_views(index, out, copy):
        def store(part, at, tile, x):
            out[at // ROWS, at % ROWS : at % ROWS + STEP, tile] = x.astype(BF16)
        for c in range(nc):
            window(index, (2,), store, range(c * ROWS, (c + 1) * ROWS, STEP))
            copy(c).start()

    def send_aside(k):
        send_views(k + s + 1, side_out.at[k], functools.partial(copy_s, k))

    def side_phase(k):
        for c in range(nc):
            copy_s(k, c).wait_recv()
            for at in range(0, ROWS, STEP):
                sv, cv = sin_cos(side_in[k, c, at : at + STEP, :].astype(F32))
                rows = slice(c * ROWS + at, c * ROWS + at + STEP)
                tv[lax.rem(k, 2), 0, rows, :] = cv
                tv[lax.rem(k, 2), 1, rows, :] = sv

    def windows(k):
        window_b(k)
        window_f(k)

    def scatter(k):
        r, c = pos[0, 0, k + s], pos[0, 1, k + s]
        own = lane >= c
        turn = lax.rem(c, LANES)
        def lay(lo, hi):
            for at in range(lo, hi, STEP):
                rows = slice(at, at + STEP)
                sr = saved[0, 0, k, 0, rows, :].astype(F32)
                si = saved[0, 0, k, 1, rows, :].astype(F32)
                d = (bk[1, rows, :] * sr + bk[0, rows, :] * si) * -SIGMA
                d = [pltpu.roll(d[:, i * LANES : (i + 1) * LANES], turn, 1) for i in range(cols)]
                zero = jnp.zeros((STEP, LANES), F32)
                d = [zero] + d + [zero]
                for i in range(cols + 1):
                    pad[i, pl.ds(2 * (spare + at), STEP, stride=2), :] = jnp.where(own, d[i + 1], d[i])

        def add(lo, hi):
            for at in range(lo, hi, STEP):
                for i in range(cols + 1):
                    total[at : at + STEP, i * LANES : (i + 1) * LANES] += pad[
                        i, pl.ds(2 * (spare - r + at), STEP, stride=2), :
                    ]

        final = None if isinstance(k, int) else k == ticks - 1
        for side, lo, at, start in ((0, 0, 0, tile_down), (1, n - margin, margin + core, tile_up)):
            lay(lo, lo + margin)
            add(at, at + margin)
            if final is not None:
                @pl.when(final)
                def _():
                    edge_out[side] = total[at : at + margin, :].astype(BF16)
                    start(edge_out, edge_in, send_e, recv_e)
        lay(margin, n - margin)
        add(margin, margin + core)

    def send_back(k, c, lur, lui):
        rows = slice(c * ROWS, (c + 1) * ROWS)
        slot = lax.rem(k, 2)
        tr, ti = ta[slot, 0, rows, :], ta[slot, 1, rows, :]
        br = tr * lur - ti * lui
        bi = tr * lui + ti * lur
        bk[0, rows, :] = br
        bk[1, rows, :] = bi

        if isinstance(k, int):
            @pl.when(odd)
            def _():
                out_b[k, c, 0] = br.astype(BF16)
                out_b[k, c, 1] = bi.astype(BF16)
                copy_b(k, c).start()
            return

        @pl.when(odd)
        def _():
            out_b[k, c, 0] = br.astype(BF16)
            out_b[k, c, 1] = (bi * jnp.where(k == ticks - 1, -1.0, 1.0)).astype(BF16)
            pl.when(k < ticks - 1)(lambda: copy_b(k, c).start())
            pl.when(k == ticks - 1)(lambda: last_b(c).start())

    def backward(k):
        def arrived(c):
            @pl.when(jnp.logical_not(last))
            def _():
                copy_b(k - 1, c).wait_recv()

            @pl.when(jnp.logical_and(k == 1, behind))
            def _():
                copy_v(c).wait_recv()
                lur, lui = in_b[1, c, 0].astype(F32), in_b[1, c, 1].astype(F32)
                ti, tr = sin_cos(view_in[c].astype(F32))
                in_b[1, c, 0] = (tr * lur - ti * lui).astype(BF16)
                in_b[1, c, 1] = (tr * lui + ti * lur).astype(BF16)
            return stacked(in_b[k, c])

        product(m_left, arrived, main.at[1], functools.partial(send_back, k))

    def pass_on(k):
        def sink(c, lur, lui):
            rows = slice(c * ROWS, (c + 1) * ROWS)
            slot = lax.rem(k, 2)
            tr, ti = tv[slot, 0, rows, :], tv[slot, 1, rows, :]
            out_r[k, c, 0] = (tr * lur - ti * lui).astype(BF16)
            bi = tr * lui + ti * lur
            if isinstance(k, int):
                out_r[k, c, 1] = bi.astype(BF16)
                copy_r(k, c).start()
            else:
                out_r[k, c, 1] = (bi * jnp.where(k == ticks - 2, -1.0, 1.0)).astype(BF16)
                pl.when(k < ticks - 2)(lambda: copy_r(k, c).start())
                pl.when(k == ticks - 2)(lambda: last_r(c).start())

        product(m_left, lambda c: stacked(out_b[k, c]), main.at[1], sink)

    def entering(k, c, waits):
        if waits:
            @pl.when(jnp.logical_not(first))
            def _():
                copy_f(k - 1, c).wait_recv()
        rows = slice(c * ROWS, (c + 1) * ROWS)
        slot = lax.rem(k, 2)
        wr, wi = in_f[k, c, 0].astype(F32), in_f[k, c, 1].astype(F32)
        tr, ti = tf[slot, 0, rows, :], tf[slot, 1, rows, :]
        return jnp.concatenate([tr * wr - ti * wi, tr * wi + ti * wr], axis=0).astype(BF16)

    def forward(k, waits=True):
        def sink(c, outr, outi):
            out_f[k, c, 0] = outr.astype(BF16)
            out_f[k, c, 1] = outi.astype(BF16)
            copy_f(k, c).start()

        product(m_left, lambda c: entering(k, c, waits), main.at[1], sink)

    def forward_last(k, waits=True):
        def detect(c, vr, vi):
            rows = slice(c * ROWS, (c + 1) * ROWS)
            excess = vr * vr + vi * vi - inten[0, k, rows, :].astype(F32)
            y_buf[c, 0:ROWS, :] = (excess * vr).astype(BF16)
            y_buf[c, ROWS : 2 * ROWS, :] = (excess * vi).astype(BF16)

        def seed(c, outr, outi):
            in_b[k + 1, c, 0] = outr.astype(BF16)
            in_b[k + 1, c, 1] = -outi.astype(BF16)

        product(lambda o, c: l_f[o, c], lambda c: entering(k, c, waits), r_f, detect)
        product(lambda o, c: l_g[o, c], lambda c: y_buf[c], r_g, seed)

    @pl.when(ahead)
    def _():
        send_views(s, view_out, copy_v)

    @pl.when(jnp.logical_not(last))
    def _():
        pl.semaphore_wait(ready, 1)

    pl.when(aside)(lambda: send_aside(0))
    for at, side, rows in strips:
        phase_table(at, halo_in[side, rows, :].astype(F32))
    window_f(0)

    @pl.when(jnp.logical_not(last))
    def _():
        forward(0, False)

    @pl.when(last)
    def _():
        forward_last(0, False)

    window_b(0)
    for c in range(nc):
        rows = slice(c * ROWS, (c + 1) * ROWS)
        send_back(0, c, bk[0, rows, :], bk[1, rows, :])

    @pl.when(relay)
    def _():
        side_phase(0)
        pass_on(0)

    @pl.when(aside)
    def _():
        for k in range(1, ticks - 1):
            send_aside(k)

    early = jnp.logical_or(first, jnp.logical_and(odd, jnp.logical_not(last)))
    loads["saved"].wait()

    @pl.when(early)
    def _():
        window_f(1)

        def tick(k, carry):
            forward(k)

            @pl.when(k == 1)
            def _():
                window_b(1)
                pl.when(relay)(lambda: side_phase(1))
                scatter(0)
            backward(k)
            pl.when(jnp.logical_and(relay, k < ticks - 1))(lambda: pass_on(k))
            scatter(k)

            @pl.when(k < ticks - 1)
            def _():
                windows(k + 1)
            pl.when(jnp.logical_and(relay, k < ticks - 2))(lambda: side_phase(k + 1))
            return carry
        lax.fori_loop(1, ticks, tick, 0)

    @pl.when(jnp.logical_not(early))
    def _():
        windows(1)
        pl.when(relay)(lambda: side_phase(1))
        scatter(0)

        def tick(k, carry):
            backward(k)
            pl.when(jnp.logical_and(relay, k < ticks - 1))(lambda: pass_on(k))
            scatter(k)

            @pl.when(k < ticks - 1)
            def _():
                windows(k + 1)
            pl.when(jnp.logical_and(relay, k < ticks - 2))(lambda: side_phase(k + 1))

            @pl.when(jnp.logical_not(last))
            def _():
                forward(k)

            @pl.when(last)
            def _():
                forward_last(k)
            return carry
        lax.fori_loop(1, ticks, tick, 0)

    o_grad[0, margin : core - margin, :] = total[2 * margin : core, :]
    for c in range(nc):
        @pl.when(jnp.logical_not(first))
        def _():
            copy_f(ticks - 1, c).wait_recv()
        o_fwd[0, 0, :, c * ROWS : (c + 1) * ROWS, :] = in_f[ticks, c].astype(F32)
    tile_wait(edge_out, edge_in, send_e, recv_e)
    o_grad[0, 0:margin, :] = total[margin : 2 * margin, :] + edge_in[0].astype(F32)
    o_grad[0, core - margin : core, :] = total[core : core + margin, :] + edge_in[1].astype(F32)

    @pl.when(last)
    def _():
        for c in range(nc):
            rows = slice(c * ROWS, (c + 1) * ROWS)
            o_adj[0, 0, 0, rows, :] = in_b[ticks, c, 0]
            o_adj[0, 0, 1, rows, :] = -in_b[ticks, c, 1]

    @pl.when(jnp.logical_not(last))
    def _():
        for c in range(nc):
            last_b(c).wait_recv()

    for c in range(nc):
        @pl.when(ahead)
        def _():
            copy_v(c).wait_send()
            copy_b(0, c).wait_send()

        for k in range(ticks):
            pl.when(jnp.logical_not(last))(lambda: copy_f(k, c).wait_send())
            pl.when(odd)(lambda: copy_b(k, c).wait_send())
        for k in range(ticks - 1):
            pl.when(relay)(lambda: copy_r(k, c).wait_send())
            pl.when(aside)(lambda: copy_s(k, c).wait_send())


def finish(wave, adj, grad, o_wave, o_adj, o_grad, sem):
    moves = [
        pltpu.make_async_copy(src, dst, sem.at[i])
        for i, (src, dst) in enumerate(((wave, o_wave), (grad, o_grad), (adj, o_adj)))
    ]
    for move in moves:
        move.start()
    for move in moves:
        move.wait()


def on_device(sections, tiles, potential, probe, positions, intensity, fwd_wave, adj_wave, saved_wave):
    n = probe.shape[1]
    nc = n // ROWS
    ticks = intensity.shape[1]
    core, width = potential.shape[1], potential.shape[2]
    margin = (width - core) // 2
    main, ends = (jnp.asarray(x) for x in tables(n))
    held = lambda x: pltpu.VMEM(x.shape, x.dtype)
    vmem = pl.BlockSpec(memory_space=pltpu.VMEM)
    spots = jnp.swapaxes(positions, 1, 2)
    hbm = pl.BlockSpec(memory_space=pltpu.HBM)
    dma = lambda *shape: pltpu.SemaphoreType.DMA(shape)
    far = lambda x: pltpu.with_memory_space_constraint(x, pltpu.HBM)
    near = lambda x: pltpu.with_memory_space_constraint(x, pltpu.VMEM)
    wave = lambda count: pltpu.VMEM((count, nc, 2, ROWS, n), BF16)
    lt = pltpu.VMEM((nc, nc, 2 * ROWS, 2 * ROWS), BF16)
    rt = pltpu.VMEM((2 * n, 2 * n), BF16)
    square = pltpu.VMEM((width, width), F32)
    pair = pltpu.VMEM((2, 2, n, n), F32)
    view = lambda *count: pltpu.VMEM((*count, ROWS, n), BF16)
    strip = pltpu.VMEM((2, margin, width), BF16)
    wave_next, adj_next, gradient = pl.pallas_call(
        functools.partial(kernel, sections, tiles),
        out_shape=(
            pltpu.VMEM(fwd_wave.shape, F32),
            pltpu.VMEM(adj_wave.shape, BF16),
            pltpu.VMEM(potential.shape, F32),
        ),
        in_specs=[hbm] * 9,
        out_specs=(vmem, vmem, vmem),
        scratch_shapes=[
            wave(ticks + 1), wave(ticks + 1), wave(ticks), wave(ticks), wave(ticks - 1),
            held(main), lt, rt, lt, rt,
            pltpu.VMEM((width // LANES, 3 * width, LANES), F32), pair, pair, pair, pltpu.VMEM((2, n, n), F32),
            square, pltpu.VMEM((width // LANES, 4 * width - 2 * n, LANES), F32),
            pltpu.VMEM((nc, 2 * ROWS, n), BF16),
            strip, strip, strip, strip, view(nc), view(nc),
            view(ticks - 1, nc), view(ticks - 1, nc),
            pltpu.SMEM(spots.shape, spots.dtype), held(potential), held(probe), held(intensity), held(fwd_wave), held(adj_wave),
            held(saved_wave), held(ends), dma(9),
            dma(ticks, nc), dma(ticks, nc), dma(ticks, nc), dma(ticks, nc),
            dma(2), dma(2), dma(2), dma(2), dma(nc), dma(nc),
            dma(ticks - 1, nc), dma(ticks - 1, nc), dma(ticks - 1, nc), pltpu.SemaphoreType.REGULAR,
        ],
        compiler_params=pltpu.CompilerParams(
            collective_id=0, has_side_effects=True, vmem_limit_bytes=VLIM * 1024 * 1024
        ),
        name="window",
    )(
        *(far(x) for x in (spots, potential, probe, intensity, fwd_wave, adj_wave, saved_wave, main, ends)),
    )
    return pl.pallas_call(
        finish,
        out_shape=(
            jax.ShapeDtypeStruct(fwd_wave.shape, F32),
            jax.ShapeDtypeStruct(adj_wave.shape, BF16),
            jax.ShapeDtypeStruct(potential.shape, F32),
        ),
        in_specs=[vmem, vmem, vmem],
        out_specs=(hbm, hbm, hbm),
        scratch_shapes=[dma(3)],
        name="finish",
    )(near(wave_next), near(adj_next), near(gradient))


def solution(mesh):
    placed = (
        P("depth", "tile", None),
        P(),
        P("tile", None, None),
        P("tile", None, None, None),
        P("depth", "tile", None, None, None),
        P("depth", "tile", None, None, None),
        P("depth", "tile", None, None, None, None),
    )
    return jax.shard_map(
        functools.partial(on_device, mesh.shape["depth"], mesh.shape["tile"]),
        mesh=mesh,
        in_specs=placed,
        out_specs=(
            P("depth", "tile", None, None, None),
            P("depth", "tile", None, None, None),
            P("depth", "tile", None),
        ),
        check_vma=False,
    )
```

```python
import functools
import math

import jax
import jax.numpy as jnp
import numpy as np
from jax import lax
from jax.experimental import pallas as pl
from jax.experimental.pallas import tpu as pltpu
from jax.sharding import PartitionSpec as P

SIGMA = 0.8
DEFOCUS = 6.0
VTOP = 3.0
ROWS = 128
LANES = 128
STEP = 32
VLIM = 40
MESH = pl.DeviceIdType.MESH
F32 = jnp.float32
BF16 = jnp.bfloat16


def rounded(x):
    return x.real.astype(BF16).astype(np.float64) + 1j * x.imag.astype(BF16).astype(np.float64)


def left_blocks(x):
    n = x.shape[0]
    nc = n // ROWS
    out = np.zeros((nc, nc, 2 * ROWS, 2 * ROWS))
    for o in range(nc):
        for c in range(nc):
            b = x[o * ROWS : (o + 1) * ROWS, c * ROWS : (c + 1) * ROWS]
            out[o, c] = np.block([[b.real, -b.imag], [b.imag, b.real]])
    return out.transpose(0, 2, 1, 3).reshape(2 * n, 2 * n)


def right_block(x):
    return np.block([[x.real, x.imag], [-x.imag, x.real]])


def tables(n):
    idx = np.arange(n)
    angle = (idx[:, None] * idx[None, :] % n) * (2.0 * math.pi / n)
    scale = 1.0 / math.sqrt(n)
    cos_t = np.asarray((np.cos(angle) * scale).astype(BF16)).astype(np.float64)
    sin_t = np.asarray((np.sin(angle) * scale).astype(BF16)).astype(np.float64)
    freq = np.where(idx < n // 2, idx, idx - n).astype(np.float64)
    q = np.exp(-1j * math.pi * DEFOCUS * freq * freq / (n * n))
    f = cos_t - 1j * sin_t
    m = (np.conj(f) * q[None, :]) @ f
    m = (m + m.T) / 2
    best = (np.inf, 1.0)
    for size in np.linspace(0.7, 1.4, 64):
        z = (size * np.exp(1j * np.linspace(0.0, math.pi / 2, 128, endpoint=False)))[:, None]
        row = m[0][None, :]
        miss = np.sum(np.abs(rounded(row * z) - row * z) ** 2, axis=1) / size**2
        miss += np.sum(np.abs(rounded(row / z) - row / z) ** 2, axis=1) * size**2
        at = int(np.argmin(miss))
        if miss[at] < best[0]:
            best = (miss[at], z[at, 0])
    z = best[1]
    g = np.conj(f) * q[None, :]
    main = np.stack([left_blocks(z * m), right_block(m / z)]).astype(BF16)
    ends = [p for v in (f, g, g.T) for p in (v.real, v.imag)]
    return main, np.stack(ends).astype(BF16)


def sin_cos(v):
    mid = 0.5 * VTOP * SIGMA
    y = v * SIGMA - mid
    z = y * y
    s = y * (1.0 + z * (-1.0 / 6 + z * (1.0 / 120 + z * (-1.0 / 5040 + z * (1.0 / 362880)))))
    c = 1.0 + z * (-0.5 + z * (1.0 / 24 + z * (-1.0 / 720 + z * (1.0 / 40320))))
    sm, cm = math.sin(mid), math.cos(mid)
    return s * cm + c * sm, c * cm - s * sm


def dot(a, b):
    return jnp.dot(a, b, preferred_element_type=F32)


def kernel(
    sections, tiles,
    pos_h, pot_h, probe_h, inten_h, fwd_h, adj_h, saved_h, main_h, ends_h,
    o_fwd, o_adj, o_grad,
    in_f, in_b, out_f, out_b, out_r, main, l_f, r_f, l_g, r_g,
    cs, tf, ta, tv, bk, total, pad, y_buf,
    halo_out, halo_in, edge_out, edge_in, view_out, view_in, side_out, side_in,
    pos, pot, probe, inten, fwd, adj, saved, ends, load_sem,
    send_f, recv_f, send_b, recv_b, send_h, recv_h, send_e, recv_e, send_v, recv_v, send_r, send_s, recv_s, ready,
):
    n = probe.shape[1]
    nc = n // ROWS
    cols = n // LANES
    core, width = pot.shape[1], pot.shape[2]
    margin = (width - core) // 2
    ticks = inten.shape[1]
    s = lax.axis_index("depth")
    t = lax.axis_index("tile")
    first, last = s == 0, s == sections - 1
    low, high = t == 0, t == tiles - 1
    odd = lax.rem(s, 2) == 1
    relay = jnp.logical_and(odd, s > 1)
    aside = jnp.logical_and(jnp.logical_not(odd), jnp.logical_and(s > 0, s < sections - 1))
    ahead = jnp.logical_and(lax.rem(s, 2) == 0, s > 0)
    behind = jnp.logical_and(lax.rem(s, 2) == 1, s < sections - 1)

    loads = {}

    def load(name, src, dst):
        loads[name] = pltpu.make_async_copy(src, dst, load_sem.at[len(loads)])
        return loads[name]

    barrier = pltpu.get_barrier_semaphore()
    one = lambda c: jnp.where(c, 1, 0).astype(jnp.int32)

    def greet(cond, axis, to):
        @pl.when(cond)
        def _():
            pl.semaphore_signal(barrier, inc=1, device_id={axis: to}, device_id_type=MESH)

    greet(t > 0, "tile", t - 1)
    greet(t < tiles - 1, "tile", t + 1)
    greet(s < sections - 1, "depth", s + 1)
    greet(jnp.logical_and(odd, s < sections - 2), "depth", s + 2)
    load("pot", pot_h, pot).start()
    load("pos", pos_h, pos).start()
    load("main", main_h, main).start()
    load("adj", adj_h, adj).start()
    load("fwd", fwd_h, fwd).start()
    load("probe", probe_h, probe)
    load("ends", ends_h, ends)
    load("inten", inten_h, inten)

    @pl.when(first)
    def _():
        loads["probe"].start()

    @pl.when(last)
    def _():
        loads["ends"].start()
        loads["inten"].start()

    load("saved", saved_h, saved).start()
    loads["pot"].wait()
    halo_out[0] = pot[0, 0:margin, :].astype(BF16)
    halo_out[1] = pot[0, core - margin : core, :].astype(BF16)
    pl.semaphore_wait(barrier, one(s > 0) + one(relay) + one(t > 0) + one(t < tiles - 1))

    def hop(src, dst, ssem, rsem, axis, to):
        return pltpu.make_async_remote_copy(
            src_ref=src, dst_ref=dst, send_sem=ssem, recv_sem=rsem,
            device_id={axis: to}, device_id_type=MESH,
        )

    def tile_pair(src, dst, ssem, rsem):
        down = hop(src.at[0], dst.at[1], ssem.at[0], rsem.at[1], "tile", t - 1)
        up = hop(src.at[1], dst.at[0], ssem.at[1], rsem.at[0], "tile", t + 1)
        return down, up

    def tile_down(*refs):
        pl.when(t > 0)(tile_pair(*refs)[0].start)

    def tile_up(*refs):
        pl.when(t < tiles - 1)(tile_pair(*refs)[1].start)

    def tile_start(src, dst, ssem, rsem):
        tile_down(src, dst, ssem, rsem)
        tile_up(src, dst, ssem, rsem)

    def tile_wait(src, dst, ssem, rsem):
        down, up = tile_pair(src, dst, ssem, rsem)

        @pl.when(t > 0)
        def _():
            down.wait_send()
            up.wait_recv()

        @pl.when(t < tiles - 1)
        def _():
            up.wait_send()
            down.wait_recv()

    tile_start(halo_out, halo_in, send_h, recv_h)

    @pl.when(s > 0)
    def _():
        pl.semaphore_signal(ready, inc=1, device_id={"depth": s - 1}, device_id_type=MESH)

    def stacked(x):
        return x.reshape(2 * ROWS, n)

    def m_left(o, c):
        return main[0, o * 2 * ROWS : (o + 1) * 2 * ROWS, c * 2 * ROWS : (c + 1) * 2 * ROWS]

    def product(get_left, get_x, r_ref, sink):
        acc = [None] * nc
        for c in range(nc):
            x = get_x(c)
            for o in range(nc):
                term = dot(get_left(o, c), x)
                acc[o] = term if acc[o] is None else acc[o] + term
        for o in range(nc):
            a = acc[o].astype(BF16)
            out = dot(jnp.concatenate([a[0:ROWS, :], a[ROWS : 2 * ROWS, :]], axis=1), r_ref[...])
            sink(o, out[:, 0:n], out[:, n : 2 * n])

    def copy_f(k, c):
        return hop(out_f.at[k, c], in_f.at[k + 1, c], send_f.at[k, c], recv_f.at[k, c], "depth", s + 1)

    def copy_b(k, c):
        return hop(out_b.at[k, c], in_b.at[k + 1, c], send_b.at[k, c], recv_b.at[k, c], "depth", s - 1)

    def copy_r(k, c):
        return hop(out_r.at[k, c], in_b.at[k + 2, c], send_r.at[k, c], recv_b.at[k + 1, c], "depth", s - 2)

    def last_r(c):
        k, rows = ticks - 2, slice(c * ROWS, (c + 1) * ROWS)
        return hop(out_r.at[k, c], o_adj.at[0, 0, :, rows, :], send_r.at[k, c], recv_b.at[k + 1, c], "depth", s - 2)

    def copy_s(k, c):
        return hop(side_out.at[k, c], side_in.at[k, c], send_s.at[k, c], recv_s.at[k, c], "depth", s + 1)

    def last_b(c):
        k, rows = ticks - 1, slice(c * ROWS, (c + 1) * ROWS)
        return hop(out_b.at[k, c], o_adj.at[0, 0, :, rows, :], send_b.at[k, c], recv_b.at[k, c], "depth", s - 1)

    loads["adj"].wait()
    for c in range(nc):
        rows = slice(c * ROWS, (c + 1) * ROWS)
        in_b[0, c, 0] = adj[0, 0, 0, rows, :]
        in_b[0, c, 1] = -adj[0, 0, 1, rows, :]
    loads["main"].wait()

    def keep(o, lur, lui):
        rows = slice(o * ROWS, (o + 1) * ROWS)
        bk[0, rows, :] = lur
        bk[1, rows, :] = lui
        out_b[0, o, 0] = lur.astype(BF16)
        out_b[0, o, 1] = lui.astype(BF16)
        pl.when(ahead)(lambda: copy_b(0, o).start())

    product(m_left, lambda c: stacked(in_b[0, c]), main.at[1], keep)

    def place(part, at, x):
        for i in range(cols + 1):
            cs[i, pl.ds(3 * at + part, STEP, stride=3), :] = x[:, i * LANES : (i + 1) * LANES]

    def phase_table(at, v):
        sv, cv = sin_cos(v)
        place(0, at, cv)
        place(1, at, sv)

    for at in range(0, core, STEP):
        place(2, margin + at, pot[0, at : at + STEP, :])
        phase_table(margin + at, pot[0, at : at + STEP, :])
    total[...] = jnp.zeros_like(total)
    spare = width - n
    for i in range(cols + 1):
        pad[i, 0 : 2 * spare, :] = jnp.zeros((2 * spare, LANES), F32)
        pad[i, 2 * (spare + n) : 2 * (2 * spare + n), :] = jnp.zeros((2 * spare, LANES), F32)
    loads["fwd"].wait()
    for c in range(nc):
        rows = slice(c * ROWS, (c + 1) * ROWS)
        for part in range(2):
            in_f[0, c, part] = fwd[0, 0, part, rows, :].astype(BF16)

    @pl.when(first)
    def _():
        loads["probe"].wait()
        for k in range(ticks):
            for c in range(nc):
                for part in range(2):
                    in_f[k + 1, c, part] = probe[part, c * ROWS : (c + 1) * ROWS, :]

    @pl.when(last)
    def _():
        loads["ends"].wait()
        loads["inten"].wait()

        def fill_left(ref, xr, xi):
            for o in range(nc):
                for c in range(nc):
                    br = xr[o * ROWS : (o + 1) * ROWS, c * ROWS : (c + 1) * ROWS]
                    bi = xi[o * ROWS : (o + 1) * ROWS, c * ROWS : (c + 1) * ROWS]
                    ref[o, c, 0:ROWS, 0:ROWS] = br
                    ref[o, c, 0:ROWS, ROWS : 2 * ROWS] = -bi
                    ref[o, c, ROWS : 2 * ROWS, 0:ROWS] = bi
                    ref[o, c, ROWS : 2 * ROWS, ROWS : 2 * ROWS] = br

        def fill_right(ref, xr, xi):
            ref[0:n, 0:n] = xr
            ref[0:n, n : 2 * n] = xi
            ref[n : 2 * n, 0:n] = -xi
            ref[n : 2 * n, n : 2 * n] = xr

        fill_left(l_f, ends[0], ends[1])
        fill_right(r_f, ends[0], ends[1])
        fill_left(l_g, ends[2], ends[3])
        fill_right(r_g, ends[4], ends[5])

    @pl.when(low)
    def _():
        halo_in[0] = jnp.zeros((margin, width), BF16)
        edge_in[0] = jnp.zeros((margin, width), BF16)

    @pl.when(high)
    def _():
        halo_in[1] = jnp.zeros((margin, width), BF16)
        edge_in[1] = jnp.zeros((margin, width), BF16)

    loads["pos"].wait()
    tile_wait(halo_out, halo_in, send_h, recv_h)
    strips = [(side * (margin + core) + at, side, slice(at, at + STEP)) for side in range(2) for at in range(0, margin, STEP)]
    for at, side, rows in strips:
        place(2, at, halo_in[side, rows, :].astype(F32))

    lane = lax.broadcasted_iota(jnp.int32, (STEP, LANES), 1)

    def window(index, parts, store, steps=range(0, n, STEP)):
        r, c = pos[0, 0, index], pos[0, 1, index]
        turn = lax.rem(LANES - c, LANES)
        own = lane < LANES - c
        for part in parts:
            for at in steps:
                rows = pl.ds(3 * (r + at) + part, STEP, stride=3)
                x = [pltpu.roll(cs[i, rows, :], turn, 1) for i in range(cols + 1)]
                for i in range(cols):
                    store(part, at, slice(i * LANES, (i + 1) * LANES), jnp.where(own, x[i], x[i + 1]))

    def window_b(k):
        def store(part, at, tile, x):
            ta[lax.rem(k, 2), part, at : at + STEP, tile] = x
        window(k + s, range(2), store)

    def window_f(k):
        def store(part, at, tile, x):
            tf[lax.rem(k, 2), part, at : at + STEP, tile] = x
        window(k - s + 2 * sections - 1, range(2), store)

    def copy_v(c):
        return hop(view_out.at[c], view_in.at[c], send_v.at[c], recv_v.at[c], "depth", s - 1)

    def send_views(index, out, copy):
        def store(part, at, tile, x):
            out[at // ROWS, at % ROWS : at % ROWS + STEP, tile] = x.astype(BF16)
        for c in range(nc):
            window(index, (2,), store, range(c * ROWS, (c + 1) * ROWS, STEP))
            copy(c).start()

    def send_aside(k):
        send_views(k + s + 1, side_out.at[k], functools.partial(copy_s, k))

    def side_phase(k):
        for c in range(nc):
            copy_s(k, c).wait_recv()
            for at in range(0, ROWS, STEP):
                sv, cv = sin_cos(side_in[k, c, at : at + STEP, :].astype(F32))
                rows = slice(c * ROWS + at, c * ROWS + at + STEP)
                tv[lax.rem(k, 2), 0, rows, :] = cv
                tv[lax.rem(k, 2), 1, rows, :] = sv

    def windows(k):
        window_b(k)
        window_f(k)

    def scatter(k):
        r, c = pos[0, 0, k + s], pos[0, 1, k + s]
        own = lane >= c
        turn = lax.rem(c, LANES)
        def lay(lo, hi):
            for at in range(lo, hi, STEP):
                rows = slice(at, at + STEP)
                sr = saved[0, 0, k, 0, rows, :].astype(F32)
                si = saved[0, 0, k, 1, rows, :].astype(F32)
                d = (bk[1, rows, :] * sr + bk[0, rows, :] * si) * -SIGMA
                d = [pltpu.roll(d[:, i * LANES : (i + 1) * LANES], turn, 1) for i in range(cols)]
                zero = jnp.zeros((STEP, LANES), F32)
                d = [zero] + d + [zero]
                for i in range(cols + 1):
                    pad[i, pl.ds(2 * (spare + at), STEP, stride=2), :] = jnp.where(own, d[i + 1], d[i])

        def add(lo, hi):
            for at in range(lo, hi, STEP):
                for i in range(cols + 1):
                    total[at : at + STEP, i * LANES : (i + 1) * LANES] += pad[
                        i, pl.ds(2 * (spare - r + at), STEP, stride=2), :
                    ]

        final = None if isinstance(k, int) else k == ticks - 1
        for side, lo, at, start in ((0, 0, 0, tile_down), (1, n - margin, margin + core, tile_up)):
            lay(lo, lo + margin)
            add(at, at + margin)
            if final is not None:
                @pl.when(final)
                def _():
                    edge_out[side] = total[at : at + margin, :].astype(BF16)
                    start(edge_out, edge_in, send_e, recv_e)
        lay(margin, n - margin)
        add(margin, margin + core)

    def send_back(k, c, lur, lui):
        rows = slice(c * ROWS, (c + 1) * ROWS)
        slot = lax.rem(k, 2)
        tr, ti = ta[slot, 0, rows, :], ta[slot, 1, rows, :]
        br = tr * lur - ti * lui
        bi = tr * lui + ti * lur
        bk[0, rows, :] = br
        bk[1, rows, :] = bi

        if isinstance(k, int):
            @pl.when(odd)
            def _():
                out_b[k, c, 0] = br.astype(BF16)
                out_b[k, c, 1] = bi.astype(BF16)
                copy_b(k, c).start()
            return

        @pl.when(odd)
        def _():
            out_b[k, c, 0] = br.astype(BF16)
            out_b[k, c, 1] = (bi * jnp.where(k == ticks - 1, -1.0, 1.0)).astype(BF16)
            pl.when(k < ticks - 1)(lambda: copy_b(k, c).start())
            pl.when(k == ticks - 1)(lambda: last_b(c).start())

    def backward(k):
        def arrived(c):
            @pl.when(jnp.logical_not(last))
            def _():
                copy_b(k - 1, c).wait_recv()

            @pl.when(jnp.logical_and(k == 1, behind))
            def _():
                copy_v(c).wait_recv()
                lur, lui = in_b[1, c, 0].astype(F32), in_b[1, c, 1].astype(F32)
                ti, tr = sin_cos(view_in[c].astype(F32))
                in_b[1, c, 0] = (tr * lur - ti * lui).astype(BF16)
                in_b[1, c, 1] = (tr * lui + ti * lur).astype(BF16)
            return stacked(in_b[k, c])

        product(m_left, arrived, main.at[1], functools.partial(send_back, k))

    def pass_on(k):
        def sink(c, lur, lui):
            rows = slice(c * ROWS, (c + 1) * ROWS)
            slot = lax.rem(k, 2)
            tr, ti = tv[slot, 0, rows, :], tv[slot, 1, rows, :]
            out_r[k, c, 0] = (tr * lur - ti * lui).astype(BF16)
            bi = tr * lui + ti * lur
            if isinstance(k, int):
                out_r[k, c, 1] = bi.astype(BF16)
                copy_r(k, c).start()
            else:
                out_r[k, c, 1] = (bi * jnp.where(k == ticks - 2, -1.0, 1.0)).astype(BF16)
                pl.when(k < ticks - 2)(lambda: copy_r(k, c).start())
                pl.when(k == ticks - 2)(lambda: last_r(c).start())

        product(m_left, lambda c: stacked(out_b[k, c]), main.at[1], sink)

    def entering(k, c, waits):
        if waits:
            @pl.when(jnp.logical_not(first))
            def _():
                copy_f(k - 1, c).wait_recv()
        rows = slice(c * ROWS, (c + 1) * ROWS)
        slot = lax.rem(k, 2)
        wr, wi = in_f[k, c, 0].astype(F32), in_f[k, c, 1].astype(F32)
        tr, ti = tf[slot, 0, rows, :], tf[slot, 1, rows, :]
        return jnp.concatenate([tr * wr - ti * wi, tr * wi + ti * wr], axis=0).astype(BF16)

    def forward(k, waits=True):
        def sink(c, outr, outi):
            out_f[k, c, 0] = outr.astype(BF16)
            out_f[k, c, 1] = outi.astype(BF16)
            copy_f(k, c).start()

        product(m_left, lambda c: entering(k, c, waits), main.at[1], sink)

    def forward_last(k, waits=True):
        def detect(c, vr, vi):
            rows = slice(c * ROWS, (c + 1) * ROWS)
            excess = vr * vr + vi * vi - inten[0, k, rows, :].astype(F32)
            y_buf[c, 0:ROWS, :] = (excess * vr).astype(BF16)
            y_buf[c, ROWS : 2 * ROWS, :] = (excess * vi).astype(BF16)

        def seed(c, outr, outi):
            in_b[k + 1, c, 0] = outr.astype(BF16)
            in_b[k + 1, c, 1] = -outi.astype(BF16)

        product(lambda o, c: l_f[o, c], lambda c: entering(k, c, waits), r_f, detect)
        product(lambda o, c: l_g[o, c], lambda c: y_buf[c], r_g, seed)

    @pl.when(ahead)
    def _():
        send_views(s, view_out, copy_v)

    @pl.when(jnp.logical_not(last))
    def _():
        pl.semaphore_wait(ready, 1)

    pl.when(aside)(lambda: send_aside(0))
    for at, side, rows in strips:
        phase_table(at, halo_in[side, rows, :].astype(F32))
    window_f(0)

    @pl.when(jnp.logical_not(last))
    def _():
        forward(0, False)

    @pl.when(last)
    def _():
        forward_last(0, False)

    window_b(0)
    for c in range(nc):
        rows = slice(c * ROWS, (c + 1) * ROWS)
        send_back(0, c, bk[0, rows, :], bk[1, rows, :])

    @pl.when(relay)
    def _():
        side_phase(0)
        pass_on(0)

    @pl.when(aside)
    def _():
        for k in range(1, ticks - 1):
            send_aside(k)

    early = jnp.logical_or(first, jnp.logical_and(odd, jnp.logical_not(last)))
    loads["saved"].wait()

    @pl.when(early)
    def _():
        window_f(1)

        def tick(k, carry):
            forward(k)

            @pl.when(k == 1)
            def _():
                window_b(1)
                pl.when(relay)(lambda: side_phase(1))
                scatter(0)
            backward(k)
            pl.when(jnp.logical_and(relay, k < ticks - 1))(lambda: pass_on(k))
            scatter(k)

            @pl.when(k < ticks - 1)
            def _():
                windows(k + 1)
            pl.when(jnp.logical_and(relay, k < ticks - 2))(lambda: side_phase(k + 1))
            return carry
        lax.fori_loop(1, ticks, tick, 0)

    @pl.when(jnp.logical_not(early))
    def _():
        windows(1)
        pl.when(relay)(lambda: side_phase(1))
        scatter(0)

        def tick(k, carry):
            backward(k)
            pl.when(jnp.logical_and(relay, k < ticks - 1))(lambda: pass_on(k))
            scatter(k)

            @pl.when(k < ticks - 1)
            def _():
                windows(k + 1)
            pl.when(jnp.logical_and(relay, k < ticks - 2))(lambda: side_phase(k + 1))

            @pl.when(jnp.logical_not(last))
            def _():
                forward(k)

            @pl.when(last)
            def _():
                forward_last(k)
            return carry
        lax.fori_loop(1, ticks, tick, 0)

    o_grad[0, margin : core - margin, :] = total[2 * margin : core, :]
    for c in range(nc):
        @pl.when(jnp.logical_not(first))
        def _():
            copy_f(ticks - 1, c).wait_recv()
        o_fwd[0, 0, :, c * ROWS : (c + 1) * ROWS, :] = in_f[ticks, c].astype(F32)
    tile_wait(edge_out, edge_in, send_e, recv_e)
    o_grad[0, 0:margin, :] = total[margin : 2 * margin, :] + edge_in[0].astype(F32)
    o_grad[0, core - margin : core, :] = total[core : core + margin, :] + edge_in[1].astype(F32)

    @pl.when(last)
    def _():
        for c in range(nc):
            rows = slice(c * ROWS, (c + 1) * ROWS)
            o_adj[0, 0, 0, rows, :] = in_b[ticks, c, 0]
            o_adj[0, 0, 1, rows, :] = -in_b[ticks, c, 1]

    @pl.when(jnp.logical_not(last))
    def _():
        for c in range(nc):
            last_b(c).wait_recv()

    for c in range(nc):
        @pl.when(ahead)
        def _():
            copy_v(c).wait_send()
            copy_b(0, c).wait_send()

        for k in range(ticks):
            pl.when(jnp.logical_not(last))(lambda: copy_f(k, c).wait_send())
            pl.when(odd)(lambda: copy_b(k, c).wait_send())
        for k in range(ticks - 1):
            pl.when(relay)(lambda: copy_r(k, c).wait_send())
            pl.when(aside)(lambda: copy_s(k, c).wait_send())


def finish(wave, adj, grad, o_wave, o_adj, o_grad, sem):
    moves = [
        pltpu.make_async_copy(src, dst, sem.at[i])
        for i, (src, dst) in enumerate(((wave, o_wave), (grad, o_grad), (adj, o_adj)))
    ]
    for move in moves:
        move.start()
    for move in moves:
        move.wait()


def on_device(sections, tiles, potential, probe, positions, intensity, fwd_wave, adj_wave, saved_wave):
    n = probe.shape[1]
    nc = n // ROWS
    ticks = intensity.shape[1]
    core, width = potential.shape[1], potential.shape[2]
    margin = (width - core) // 2
    main, ends = (jnp.asarray(x) for x in tables(n))
    held = lambda x: pltpu.VMEM(x.shape, x.dtype)
    vmem = pl.BlockSpec(memory_space=pltpu.VMEM)
    spots = jnp.swapaxes(positions, 1, 2)
    hbm = pl.BlockSpec(memory_space=pltpu.HBM)
    dma = lambda *shape: pltpu.SemaphoreType.DMA(shape)
    far = lambda x: pltpu.with_memory_space_constraint(x, pltpu.HBM)
    near = lambda x: pltpu.with_memory_space_constraint(x, pltpu.VMEM)
    wave = lambda count: pltpu.VMEM((count, nc, 2, ROWS, n), BF16)
    lt = pltpu.VMEM((nc, nc, 2 * ROWS, 2 * ROWS), BF16)
    rt = pltpu.VMEM((2 * n, 2 * n), BF16)
    square = pltpu.VMEM((width, width), F32)
    pair = pltpu.VMEM((2, 2, n, n), F32)
    view = lambda *count: pltpu.VMEM((*count, ROWS, n), BF16)
    strip = pltpu.VMEM((2, margin, width), BF16)
    wave_next, adj_next, gradient = pl.pallas_call(
        functools.partial(kernel, sections, tiles),
        out_shape=(
            pltpu.VMEM(fwd_wave.shape, F32),
            pltpu.VMEM(adj_wave.shape, BF16),
            pltpu.VMEM(potential.shape, F32),
        ),
        in_specs=[hbm] * 9,
        out_specs=(vmem, vmem, vmem),
        scratch_shapes=[
            wave(ticks + 1), wave(ticks + 1), wave(ticks), wave(ticks), wave(ticks - 1),
            held(main), lt, rt, lt, rt,
            pltpu.VMEM((width // LANES, 3 * width + 8, LANES), F32), pair, pair, pair, pltpu.VMEM((2, n, n), F32),
            square, pltpu.VMEM((width // LANES, 4 * width - 2 * n + 8, LANES), F32),
            pltpu.VMEM((nc, 2 * ROWS, n), BF16),
            strip, strip, strip, strip, view(nc), view(nc),
            view(ticks - 1, nc), view(ticks - 1, nc),
            pltpu.SMEM(spots.shape, spots.dtype), held(potential), held(probe), held(intensity), held(fwd_wave), held(adj_wave),
            held(saved_wave), held(ends), dma(9),
            dma(ticks, nc), dma(ticks, nc), dma(ticks, nc), dma(ticks, nc),
            dma(2), dma(2), dma(2), dma(2), dma(nc), dma(nc),
            dma(ticks - 1, nc), dma(ticks - 1, nc), dma(ticks - 1, nc), pltpu.SemaphoreType.REGULAR,
        ],
        compiler_params=pltpu.CompilerParams(
            collective_id=0, has_side_effects=True, vmem_limit_bytes=VLIM * 1024 * 1024
        ),
        name="window",
    )(
        *(far(x) for x in (spots, potential, probe, intensity, fwd_wave, adj_wave, saved_wave, main, ends)),
    )
    return pl.pallas_call(
        finish,
        out_shape=(
            jax.ShapeDtypeStruct(fwd_wave.shape, F32),
            jax.ShapeDtypeStruct(adj_wave.shape, BF16),
            jax.ShapeDtypeStruct(potential.shape, F32),
        ),
        in_specs=[vmem, vmem, vmem],
        out_specs=(hbm, hbm, hbm),
        scratch_shapes=[dma(3)],
        name="finish",
    )(near(wave_next), near(adj_next), near(gradient))


def solution(mesh):
    placed = (
        P("depth", "tile", None),
        P(),
        P("tile", None, None),
        P("tile", None, None, None),
        P("depth", "tile", None, None, None),
        P("depth", "tile", None, None, None),
        P("depth", "tile", None, None, None, None),
    )
    return jax.shard_map(
        functools.partial(on_device, mesh.shape["depth"], mesh.shape["tile"]),
        mesh=mesh,
        in_specs=placed,
        out_specs=(
            P("depth", "tile", None, None, None),
            P("depth", "tile", None, None, None),
            P("depth", "tile", None),
        ),
        check_vma=False,
    )
```
